128 devices in a mesh: sx: 8 (over x, core), sy: 8 (over z, y_hi), dp: 2 (over y_lo).
Axes of the slice: x: 4, y: 4 (y_hi: 2, y_lo: 2; y = y_hi * 2 + y_lo), z: 4, core: 2. Of those that a mesh axis runs over, the one named last changes fastest.
Arguments:
- tokens: bfloat16 [2, 32768, 1280], P('dp', ('sx', 'sy')), may hold values from -6 to 6
- lengths: int32 [2, 256], P('dp'), may hold values from 1 to 512, 32768 in all within a row
- ln_gain: float32 [1280], replicated, may hold values from 0.1 to 1.9
- w_qkv: bfloat16 [1280, 3840], P('dp'), may hold values from -4 to 4, as said below
- w_out: bfloat16 [1280, 1280], P('dp'), may hold values from -0.15625 to 0.15625
Outputs:
- hidden: bfloat16 [2, 32768, 1280], P('dp', ('sx', 'sy'))
- pooled: float32 [2, 256, 1280], P('dp')
The draws below stay inside these ranges and needn't reach their ends.
Inputs may be any that keep to these rules, and one draw needn't show every extreme that they name: The 256 lengths of a row sum to 32768; images are packed end to end in order. `w_qkv`: columns are queries, then keys, then values, each of 16 heads of 80 columns.
All inputs are finite; a program needn't handle non-finite values.
Results may differ from the reference program's by a relative error of at most 0.0051.
Values may be sent and summed in bfloat16 or wider, within the bound.
A program may use at most 128 MiB of HBM per device.

```python
import math
import jax
import jax.numpy as jnp
import numpy as np
from jax import lax

D = 1280
HEADS = 16
MAXLEN = 512
ROWS = 2
SEQ = 32768
IMAGES = 256


def draw_w_qkv(key, part):
    first = jax.random.fold_in(jax.random.fold_in(key, 11), 0)
    base = jax.random.normal(first, (D, 3 * D), jnp.float32) * D ** (-0.5)
    return jnp.clip(base, -4.0, 4.0).astype(jnp.bfloat16)


def block_levels(rng, dims, pieces, least, largest):
    def one(position, shards_of):
        steps = jax.random.uniform(jax.random.fold_in(jax.random.fold_in(rng, 6), position), (shards_of,), jnp.float32, least / len(pieces), largest / len(pieces))
        return jnp.repeat(jnp.exp(steps), dims[position] // shards_of).reshape((-1,) + (1,) * (len(dims) - position - 1))

    loudness = one(*pieces[0])
    for cut in pieces[1:]:
        loudness = loudness * one(*cut)
    return loudness


def split_up(number_of, total, limit, lean):
    portions = [(1 << 20) // math.isqrt(standing ** lean) + 1 for standing in range(2, number_of + 1)]
    spare, given = total - limit - (number_of - 1), [1] * (number_of - 1)
    while spare > 0:
        candidates = [i for i in range(number_of - 1) if given[i] < limit]
        whole, remaining = sum([portions[i] for i in candidates]), spare
        for i in candidates:
            extra = min(limit - given[i], max(1, remaining * portions[i] // whole), spare)
            given[i] = given[i] + extra
            spare = spare - extra
    return np.array([limit] + given)


def ragged_sizes(stream_key, number_of, total, limit, lean):
    if number_of == 2:
        one = jax.random.randint(stream_key, (), max(1, total - limit), min(limit, total - 1) + 1)
        return jnp.stack([one, total - one])
    sizes = jnp.asarray(split_up(number_of, total, limit, lean), jnp.int32)
    twos = (number_of - 1) // 2
    donor, taker = sizes[1:1 + 2 * twos:2], sizes[2:2 + 2 * twos:2]
    room = jnp.minimum(donor - 1, limit - taker)
    passed = jax.random.randint(jax.random.fold_in(stream_key, 1), (twos,), 0, 1 << 20) % (room + 1)
    sizes = sizes.at[1:1 + 2 * twos:2].set(donor - passed).at[2:2 + 2 * twos:2].set(taker + passed)
    return sizes[jax.random.permutation(jax.random.fold_in(stream_key, 2), number_of)]


def gaussian(stream_key, shape, scale, bound, cuts=(), held_as=jnp.bfloat16):
    result = scale * jax.random.normal(stream_key, shape, jnp.float32)
    if cuts:
        result = result * block_levels(stream_key, shape, cuts, -0.22, 0.18)
    return jnp.clip(result, -bound, bound).astype(held_as)


def setup_inputs(seed: int = 0) -> dict:
    splits = jax.random.split(jax.random.key(seed), 6)
    tokens = gaussian(splits[0], (ROWS, SEQ, D), 1.0, 6.0, ((0, 2), (1, 64)))
    lengths = jax.vmap(lambda own: ragged_sizes(own, IMAGES, SEQ, MAXLEN, 2))(jax.random.split(splits[1], ROWS)).reshape((ROWS, IMAGES)).astype(jnp.int32)
    ln_gain = jnp.clip(1.0 + 0.18 * jax.random.normal(splits[2], (D,), jnp.float32), 0.1, 1.9)
    w_qkv = draw_w_qkv(jax.random.fold_in(splits[5], 71), 0)
    w_out = gaussian(splits[4], (D, D), D ** -0.5, 0.15625, ((0, 2),))
    return {"tokens": tokens, "lengths": lengths, "ln_gain": ln_gain, "w_qkv": w_qkv, "w_out": w_out}


def image_ids(lengths, positions, total):
    offsets = jnp.cumsum(lengths) - lengths
    counted = lax.optimization_barrier(jnp.sum((offsets[None, :] <= positions[:, None]).astype(jnp.int32), axis=1)) - 1
    inside = (positions >= 0) & (positions < total)
    return jnp.where(inside, counted, -1).astype(jnp.int32)

def normalize(rows, ln_gain):
    values = rows.astype(jnp.float32)
    center = values - lax.optimization_barrier(jnp.mean(values, axis=-1, keepdims=True))
    spread = lax.optimization_barrier(jnp.mean(center * center, axis=-1, keepdims=True))
    return (center * lax.rsqrt(spread + 1e-05) * ln_gain).astype(jnp.bfloat16)

def attend(queries, keys, values, q_ids, k_ids, margin):
    length = queries.shape[0]
    heads = queries.shape[1]
    block = min(512, length)
    window = block + 2 * margin
    scale = queries.shape[2] ** (-0.5)

    def one_block(index):
        start = (index * block).astype(jnp.int32)
        q_blk = lax.dynamic_slice_in_dim(queries, start, block, 0)
        k_blk = lax.dynamic_slice_in_dim(keys, start, window, 0)
        v_blk = lax.dynamic_slice_in_dim(values, start, window, 0)
        q_lab = lax.dynamic_slice_in_dim(q_ids, start, block, 0)
        k_lab = lax.dynamic_slice_in_dim(k_ids, start, window, 0)
        allowed = q_lab[:, None] == k_lab[None, :]

        def one_head(head):
            q_head = lax.dynamic_index_in_dim(q_blk, head, 1, keepdims=False)
            k_head = lax.dynamic_index_in_dim(k_blk, head, 1, keepdims=False)
            v_head = lax.dynamic_index_in_dim(v_blk, head, 1, keepdims=False)
            scores = jnp.dot(q_head, k_head.T, preferred_element_type=jnp.float32) * scale
            scores = jnp.where(allowed, scores, -1e+30)
            top = lax.optimization_barrier(jnp.max(scores, axis=1, keepdims=True))
            weights = jnp.exp(scores - top)
            probs = (weights / lax.optimization_barrier(jnp.sum(weights, axis=1, keepdims=True))).astype(jnp.bfloat16)
            return jnp.dot(probs, v_head, preferred_element_type=jnp.float32).astype(jnp.bfloat16)
        outcome = lax.map(one_head, jnp.arange(heads, dtype=jnp.int32))
        return jnp.transpose(outcome, (1, 0, 2))
    blocks = lax.map(one_block, jnp.arange(length // block, dtype=jnp.int32))
    return blocks.reshape(length, heads, -1)

def reference(tokens, lengths, ln_gain, w_qkv, w_out):
    total = tokens.shape[1]
    width = tokens.shape[2]
    size = width // HEADS
    positions = jnp.arange(total, dtype=jnp.int32)
    extended = jnp.arange(total + 2 * MAXLEN, dtype=jnp.int32) - MAXLEN

    def one_row(pair):
        row, lens = pair
        normed = normalize(row, ln_gain)
        qkv = jnp.dot(normed, w_qkv, preferred_element_type=jnp.float32).astype(jnp.bfloat16)
        qkv = qkv.reshape(total, 3, HEADS, size)
        own_ids = image_ids(lens, positions, total)
        far_ids = image_ids(lens, extended, total)
        padding = jnp.zeros((MAXLEN, 3, HEADS, size), jnp.bfloat16)
        padded = jnp.concatenate([padding, qkv, padding], axis=0)
        context = attend(qkv[:, 0], padded[:, 1], padded[:, 2], own_ids, far_ids, MAXLEN)
        mixed = jnp.dot(context.reshape(total, width), w_out, preferred_element_type=jnp.float32)
        hidden = (row.astype(jnp.float32) + mixed).astype(jnp.bfloat16)
        onehot = (jnp.arange(IMAGES, dtype=jnp.int32)[:, None] == own_ids[None, :]).astype(jnp.bfloat16)
        sums = jnp.dot(onehot, hidden, preferred_element_type=jnp.float32)
        pooled = sums / lens.astype(jnp.float32)[:, None]
        return (hidden, pooled)
    hidden, pooled = lax.map(one_row, (tokens, lengths))
    return (hidden, pooled)
```

```python
import math

import jax
import jax.numpy as jnp
from jax import lax
from jax.experimental import pallas as pl
from jax.experimental.pallas import tpu as pltpu
from jax.sharding import PartitionSpec as P

MESH = pl.DeviceIdType.MESH
F32 = jnp.float32
BF16 = jnp.bfloat16
D = 1280
HALF = 640
N = 512
SIZE = 80
IMAGES = 256
TOTAL = 32768
SCALE = SIZE**-0.5 * math.log2(math.e)
PIECE = 80
CLASSES = (2, 3, 4, 5, 6, 9)
VMEM_LIMIT = 62 * 1024 * 1024


def places():
    sx, sy, d = lax.axis_index("sx"), lax.axis_index("sy"), lax.axis_index("dp")
    h = lax.rem(sy, 2)
    flip = sy + 1 - 2 * h
    shard = sx * 8 + sy
    onward = lax.rem(shard + 2 - 4 * h + 64, 64)
    back = lax.rem(shard - 2 + 4 * h + 64, 64)
    mate = sx + 1 - 2 * lax.rem(sx, 2)
    where = {
        "a": (sx, sy, 1 - d),
        "b": (sx, flip, 1 - d),
        "xp": (lax.rem(sx + 2, 8), sy, d),
        "xm": (lax.rem(sx + 6, 8), sy, d),
        "core": (mate, sy, d),
        "z": (onward // 8, lax.rem(onward, 8), d),
        "zb": (back // 8, lax.rem(back, 8), d),
    }
    return sx, sy, d, h, mate, where


def normalize(rows, gain):
    values = rows.astype(F32)
    center = values - jnp.mean(values, axis=-1, keepdims=True)
    spread = jnp.mean(center * center, axis=-1, keepdims=True)
    return (center * lax.rsqrt(spread + 1e-05) * gain).astype(BF16)


class Exchange:
    def __init__(self, own, other, width, sx, mate, where, send, recv):
        self.own, self.other, self.width = own, other, width
        self.sx, self.mate, self.where = sx, mate, where
        self.send, self.recv = send, recv
        self.started = []

    def rows(self, owner):
        return pl.ds(pl.multiple_of(lax.rem(owner + 8, 8) * PIECE, 16), PIECE)

    def copy(self, i, src, owner, cols, to):
        rows = self.rows(owner)
        return pltpu.make_async_remote_copy(
            src_ref=src.at[rows, cols],
            dst_ref=self.other.at[rows, cols],
            send_sem=self.send.at[i],
            recv_sem=self.recv.at[i],
            device_id=self.where[to],
            device_id_type=MESH,
        )

    def describe(self, i):
        sx, w = self.sx, self.width
        low, high, full = pl.ds(0, w // 2), pl.ds(w // 2, w // 2), pl.ds(0, w)
        table = (
            (self.own, sx, low, "a"),
            (self.own, sx, high, "b"),
            (self.other, sx, full, "xp"),
            (self.other, sx, full, "xm"),
            (self.other, sx, full, "core"),
            (self.other, sx + 2, low, "xm"),
            (self.other, sx + 2, full, "core"),
            (self.other, sx - 2, high, "xp"),
            (self.other, sx - 2, full, "core"),
            (self.other, sx + 4, full, "core"),
        )
        return self.copy(i, *table[i])

    def go(self, *which):
        for i in which:
            self.describe(i).start()

    def arrived(self, *which):
        for i in which:
            self.describe(i).wait_recv()

    def sent(self):
        for i in range(10):
            self.describe(i).wait_send()


def gather_kernel(
    tok_hbm, gain_ref, wq_hbm, wo_hbm,
    q_out, k_out, v_out, wo_out,
    tok, wq, wqo, woo, near, far, ta, tb, nrm, nrm2, acc, qs, ks, vs,
    wq_send, wq_recv, wo_send, wo_recv, h_send, h_recv, local,
):
    sx, sy, d, h, mate, where = places()
    barrier = pltpu.get_barrier_semaphore()
    for name in ("a", "b", "xp", "xm", "core", "z", "zb"):
        pl.semaphore_signal(barrier, inc=1, device_id=where[name], device_id_type=MESH)

    tok_in = pltpu.make_async_copy(tok_hbm, tok, local.at[0])
    wq_in = pltpu.make_async_copy(wq_hbm, wq, local.at[1])
    tok_in.start()
    wq_in.start()
    pl.semaphore_wait(barrier, 7)

    big = Exchange(wq_hbm, wqo, 3 * D, sx, mate, where, wq_send, wq_recv)
    small = Exchange(wo_hbm, woo, D, sx, mate, where, wo_send, wo_recv)

    def chunk(i):
        return pl.ds(128 * i, 128)

    table = (
        (tok_hbm, 0, ta, 0, "a"),
        (tok_hbm, 1, ta, 1, "a"),
        (tok_hbm, 2, tb, 0, "b"),
        (tok_hbm, 3, tb, 1, "b"),
        (ta, 0, near, 0, "b"),
        (ta, 1, near, 1, "b"),
        (tb, 0, near, 2, "a"),
        (tb, 1, near, 3, "a"),
        (near, 0, far, 0, "z"),
        (near, 2, far, 2, "z"),
        (near, 1, far, 1, "z"),
        (near, 3, far, 3, "z"),
    )

    def halo(i):
        src, at, dst, to, name = table[i]
        return pltpu.make_async_remote_copy(
            src_ref=src.at[chunk(at)],
            dst_ref=dst.at[chunk(to)],
            send_sem=h_send.at[i],
            recv_sem=h_recv.at[i],
            device_id=where[name],
            device_id_type=MESH,
        )

    big.go(0, 1)
    for i in (0, 2, 1, 3):
        halo(i).start()
    small.go(0, 1)

    gain = gain_ref[...]
    mine = pl.ds(pl.multiple_of(d * HALF, 128), HALF)
    others = pl.ds(pl.multiple_of((1 - d) * HALF, 128), HALF)

    tok_in.wait()

    def norm_own(i, _):
        rows = pl.ds(pl.multiple_of(i * 64, 64), 64)
        nrm[rows, :] = normalize(tok[rows, :], gain)
        return 0

    lax.fori_loop(0, N // 64, norm_own, 0)
    wq_in.wait()

    def first_half(i, _):
        rows = pl.ds(pl.multiple_of(i * 256, 256), 256)
        for part in range(3):
            cols = pl.ds(part * D, D)
            acc[rows, cols] = jnp.dot(nrm[rows, mine], wq[:, cols], preferred_element_type=F32)
        return 0

    lax.fori_loop(0, 2, first_half, 0)

    big.arrived(0, 1)
    big.go(2, 3, 4)
    for i, j in ((0, 4), (2, 6)):
        halo(i).wait_recv()
        halo(j).start()
    big.arrived(3)
    big.go(5, 6)
    big.arrived(2)
    big.go(7, 8)
    for i, j in ((1, 5), (3, 7)):
        halo(i).wait_recv()
        halo(j).start()
    small.arrived(0, 1)
    small.go(2, 3, 4)
    big.arrived(5, 7)
    big.go(9)
    big.arrived(4, 6, 8, 9)

    def second_half(i, _):
        rows = pl.ds(pl.multiple_of(i * 256, 256), 256)
        into = pl.ds(pl.multiple_of(N + i * 256, 256), 256)
        for part, ref, at, factor in ((0, qs, rows, SCALE), (1, ks, into, None), (2, vs, into, None)):
            cols = pl.ds(part * D, D)
            value = acc[rows, cols] + jnp.dot(nrm[rows, others], wqo[:, cols], preferred_element_type=F32)
            if factor is not None:
                value = value * factor
            ref[at, :] = value.astype(BF16)
        return 0

    lax.fori_loop(0, 2, second_half, 0)
    outs = []

    def put(src, dst, start, rows, i):
        span = pl.ds(start, rows)
        copy = pltpu.make_async_copy(src.at[span], dst.at[span], local.at[i])
        copy.start()
        outs.append(copy)

    put(qs, q_out, 0, N, 2)
    put(ks, k_out, N, N, 3)
    put(vs, v_out, N, N, 4)

    near_at = (1 - h) * (2 * N)
    far_at = h * (2 * N)

    def keyvals(src, first, base, slot):
        for j in range(4):
            rows = src[pl.ds(128 * (first + 2 * (j // 2)) + 64 * (j % 2), 64), :]
            nrm2[pl.ds(64 * j, 64), :] = normalize(rows, gain)
        for part, ref, out, sem in ((1, ks, k_out, slot), (2, vs, v_out, slot + 2)):
            cols = pl.ds(part * D, D)
            value = jnp.dot(nrm2[:, mine], wq[:, cols], preferred_element_type=F32)
            value = value + jnp.dot(nrm2[:, others], wqo[:, cols], preferred_element_type=F32)
            for j in range(2):
                start = pl.multiple_of(base + 128 * (first + 2 * j), 128)
                ref[pl.ds(start, 128), :] = value[128 * j : 128 * j + 128].astype(BF16)
                put(ref, out, start, 128, sem + j)

    halo(4).wait_recv()
    halo(8).start()
    halo(6).wait_recv()
    halo(9).start()
    keyvals(near, 0, near_at, 5)
    small.arrived(3)
    small.go(5, 6)
    small.arrived(2)
    small.go(7, 8)
    halo(5).wait_recv()
    halo(10).start()
    halo(7).wait_recv()
    halo(11).start()
    keyvals(near, 1, near_at, 9)
    small.arrived(5, 7)
    small.go(9)
    halo(8).wait_recv()
    halo(9).wait_recv()
    keyvals(far, 0, far_at, 13)
    small.arrived(4, 6, 8, 9)
    wo_done = pltpu.make_async_copy(woo, wo_out, local.at[21])
    wo_done.start()
    halo(10).wait_recv()
    halo(11).wait_recv()
    keyvals(far, 1, far_at, 17)
    for copy in outs:
        copy.wait()
    wo_done.wait()
    big.sent()
    small.sent()
    for i in range(12):
        halo(i).wait_send()


def gather(tokens, gain, w_qkv, w_out):
    any_ = pl.BlockSpec(memory_space=pltpu.HBM)
    vm = pl.BlockSpec(memory_space=pltpu.VMEM)
    dma = pltpu.SemaphoreType.DMA
    return pl.pallas_call(
        gather_kernel,
        name="gather",
        out_shape=(
            jax.ShapeDtypeStruct((N, D), BF16),
            jax.ShapeDtypeStruct((3 * N, D), BF16),
            jax.ShapeDtypeStruct((3 * N, D), BF16),
            jax.ShapeDtypeStruct((HALF, D), BF16),
        ),
        in_specs=[any_, vm, any_, any_],
        out_specs=(any_,) * 4,
        scratch_shapes=[
            pltpu.VMEM((N, D), BF16),
            pltpu.VMEM((HALF, 3 * D), BF16),
            pltpu.VMEM((HALF, 3 * D), BF16),
            pltpu.VMEM((HALF, D), BF16),
            pltpu.VMEM((N, D), BF16),
            pltpu.VMEM((N, D), BF16),
            pltpu.VMEM((256, D), BF16),
            pltpu.VMEM((256, D), BF16),
            pltpu.VMEM((N, D), BF16),
            pltpu.VMEM((256, D), BF16),
            pltpu.VMEM((N, 3 * D), F32),
            pltpu.VMEM((N, D), BF16),
            pltpu.VMEM((3 * N, D), BF16),
            pltpu.VMEM((3 * N, D), BF16),
            dma((10,)),
            dma((10,)),
            dma((10,)),
            dma((10,)),
            dma((12,)),
            dma((12,)),
            dma((22,)),
        ],
        compiler_params=pltpu.CompilerParams(
            collective_id=0, has_side_effects=True, vmem_limit_bytes=VMEM_LIMIT
        ),
    )(tokens, gain, w_qkv, w_out)


def attend_kernel(
    lens_ref, q_hbm, k_hbm, v_hbm, tok_hbm, wa_hbm, wb_hbm,
    hid_hbm, part_ref,
    q, k, v, tok, wa, wb, ctx, bias, hid, qid, kid, sems,
):
    sx, sy, d = lax.axis_index("sx"), lax.axis_index("sy"), lax.axis_index("dp")
    copies = [
        pltpu.make_async_copy(a, b, sems.at[i])
        for i, (a, b) in enumerate(
            ((q_hbm, q), (k_hbm, k), (v_hbm, v), (tok_hbm, tok), (wa_hbm, wa), (wb_hbm, wb))
        )
    ]
    for copy in copies:
        copy.start()
    first = (sx * 8 + sy) * N
    base = first - N

    lens = lens_ref[...].astype(F32)
    down = lax.broadcasted_iota(jnp.int32, (IMAGES, IMAGES), 0)
    along = lax.broadcasted_iota(jnp.int32, (IMAGES, IMAGES), 1)
    wide = jnp.broadcast_to(lens, (IMAGES, IMAGES))
    off_col = jnp.sum(jnp.where(along < down, wide, 0.0), axis=1, keepdims=True)
    len_col = jnp.sum(jnp.where(along == down, wide, 0.0), axis=1, keepdims=True)
    off_row = jnp.sum(
        jnp.where(down < along, jnp.broadcast_to(len_col, (IMAGES, IMAGES)), 0.0), axis=0, keepdims=True
    )
    for j in range(3):
        pos = (lax.broadcasted_iota(jnp.int32, (1, N), 1) + (base + j * N)).astype(F32)
        count = jnp.sum(jnp.where(off_col <= pos, 1.0, 0.0), axis=0, keepdims=True) - 1.0
        kid[:, pl.ds(j * N, N)] = jnp.where(pos < TOTAL, count, -1.0)
    for j in range(4):
        pos = (lax.broadcasted_iota(jnp.int32, (128, 1), 0) + (first + j * 128)).astype(F32)
        qid[pl.ds(j * 128, 128), :] = jnp.sum(jnp.where(off_row <= pos, 1.0, 0.0), axis=1, keepdims=True) - 1.0

    for copy in copies[:3]:
        copy.wait()

    def block(i, _):
        rows = pl.ds(pl.multiple_of(i * 128, 128), 128)
        begin = (first + i * 128).astype(F32)
        low = jnp.max(jnp.where(off_row <= begin, off_row, 0.0)).astype(jnp.int32)
        high = jnp.min(jnp.where(off_row > begin + 127.0, off_row, float(TOTAL))).astype(jnp.int32)
        low = (low - base) >> 7
        high = (high - base + 127) >> 7
        blocks = high - low
        ids = qid[rows, :]
        before = 0
        for size in CLASSES:
            n = size * 128

            @pl.when((blocks > before) & (blocks <= size))
            def _():
                start = pl.multiple_of(jnp.minimum(low, 12 - size) * 128, 128)
                keys = pl.ds(start, n)
                bias[:, pl.ds(0, n)] = jnp.where(ids == kid[:, keys], 0.0, -1e30)

                def two_pairs(pp, _):
                    for sub in range(2):
                        pair = pp * 2 + sub
                        tile = (pair * 5) >> 2
                        lanes = pl.ds(pl.multiple_of(tile * 128, 128), 256)
                        shift = pair * 160 - tile * 128
                        lane = lax.broadcasted_iota(jnp.int32, (1, 256), 1) - shift
                        one = (lane >= 0) & (lane < SIZE)
                        two = (lane >= SIZE) & (lane < 2 * SIZE)
                        window = q[rows, lanes]
                        both = jnp.concatenate(
                            [
                                window * jnp.where(one, 1.0, 0.0).astype(BF16),
                                window * jnp.where(two, 1.0, 0.0).astype(BF16),
                            ],
                            axis=0,
                        )
                        scores = lax.dot_general(
                            both, k[keys, lanes], (((1,), (1,)), ((), ())), preferred_element_type=F32
                        )
                        extra = bias[:, pl.ds(0, n)]
                        scores = scores + jnp.concatenate([extra, extra], axis=0)
                        top = jnp.max(scores, axis=1, keepdims=True)
                        weights = jnp.exp2(scores - top)
                        total = jnp.sum(weights, axis=1, keepdims=True)
                        mixed = jnp.dot(weights.astype(BF16), v[keys, lanes], preferred_element_type=F32)
                        mixed = mixed * (1.0 / total)
                        old = ctx[rows, lanes].astype(F32)
                        ctx[rows, lanes] = jnp.where(one, mixed[:128], jnp.where(two, mixed[128:], old)).astype(BF16)
                    return 0

                lax.fori_loop(0, 4, two_pairs, 0)

            before = size
        return 0

    lax.fori_loop(0, 4, block, 0)
    for copy in copies[3:]:
        copy.wait()
    mine = pl.ds(pl.multiple_of(d * HALF, 128), HALF)
    others = pl.ds(pl.multiple_of((1 - d) * HALF, 128), HALF)

    def project(i, _):
        rows = pl.ds(pl.multiple_of(i * 256, 256), 256)
        mixed = jnp.dot(ctx[rows, mine], wa[...], preferred_element_type=F32)
        mixed = mixed + jnp.dot(ctx[rows, others], wb[...], preferred_element_type=F32)
        hid[rows, :] = (tok[rows, :].astype(F32) + mixed).astype(BF16)
        return 0

    lax.fori_loop(0, 2, project, 0)
    out = pltpu.make_async_copy(hid, hid_hbm, sems.at[6])
    out.start()
    image = lax.broadcasted_iota(jnp.int32, (IMAGES, 1), 0).astype(F32)
    onehot = jnp.where(image == kid[:, pl.ds(N, N)], 1.0, 0.0).astype(BF16)
    sums = jnp.dot(onehot, hid[...], preferred_element_type=F32)
    part_ref[...] = (sums / len_col).astype(BF16)
    out.wait()


def attend(lengths, q, k, v, tokens, w_own, w_other):
    any_ = pl.BlockSpec(memory_space=pltpu.HBM)
    vm = pl.BlockSpec(memory_space=pltpu.VMEM)
    return pl.pallas_call(
        attend_kernel,
        name="attend",
        out_shape=(
            jax.ShapeDtypeStruct((N, D), BF16),
            jax.ShapeDtypeStruct((IMAGES, D), BF16),
        ),
        in_specs=[vm] + [any_] * 6,
        out_specs=(any_, vm),
        scratch_shapes=[
            pltpu.VMEM((N, D), BF16),
            pltpu.VMEM((3 * N, D), BF16),
            pltpu.VMEM((3 * N, D), BF16),
            pltpu.VMEM((N, D), BF16),
            pltpu.VMEM((HALF, D), BF16),
            pltpu.VMEM((HALF, D), BF16),
            pltpu.VMEM((N, D), BF16),
            pltpu.VMEM((128, 128 * CLASSES[-1]), F32),
            pltpu.VMEM((N, D), BF16),
            pltpu.VMEM((N, 1), F32),
            pltpu.VMEM((1, 3 * N), F32),
            pltpu.SemaphoreType.DMA((7,)),
        ],
        compiler_params=pltpu.CompilerParams(vmem_limit_bytes=VMEM_LIMIT),
    )(lengths, q, k, v, tokens, w_own, w_other)


def combine_kernel(
    part, out, rc, one, rx, two, ry, three, four, last,
    c_send, c_recv, x_send, x_recv, y_send, y_recv, g_send, g_recv, w_send, w_recv,
):
    sx, sy, d = lax.axis_index("sx"), lax.axis_index("sy"), lax.axis_index("dp")
    core = lax.rem(sx, 2)
    chip = sx // 2
    mate = (sx + 1 - 2 * core, sy, d)
    chips = [(lax.rem(sx + 2 * j, 8), sy, d) for j in (1, 2, 3)]
    plane = [(sx, lax.rem(sy + j, 8), d) for j in range(1, 8)]
    barrier = pltpu.get_barrier_semaphore()
    for who in [mate] + chips + plane:
        pl.semaphore_signal(barrier, inc=1, device_id=who, device_id_type=MESH)
    pl.semaphore_wait(barrier, 11)

    def remote(src, dst, send, recv, who):
        return pltpu.make_async_remote_copy(
            src_ref=src, dst_ref=dst, send_sem=send, recv_sem=recv, device_id=who, device_id_type=MESH
        )

    my_half = pl.ds(pl.multiple_of(core * 128, 128), 128)
    its_half = pl.ds(pl.multiple_of((1 - core) * 128, 128), 128)
    c_copy = remote(part.at[its_half], rc, c_send.at[0], c_recv.at[0], mate)
    c_copy.start()
    c_copy.wait_recv()
    one[...] = (part[my_half, :].astype(F32) + rc[...].astype(F32)).astype(BF16)

    def strip(owner):
        return pl.ds(pl.multiple_of(owner * 32, 32), 32)

    x_copies = [
        remote(one.at[strip(lax.rem(chip + j, 4))], rx.at[j - 1], x_send.at[j - 1], x_recv.at[j - 1], chips[j - 1])
        for j in (1, 2, 3)
    ]
    for copy in x_copies:
        copy.start()
    for copy in x_copies:
        copy.wait_recv()
    total = one[strip(chip), :].astype(F32)
    for j in range(3):
        total = total + rx[j].astype(F32)
    for j in range(2):
        two[j] = total[:, j * HALF : (j + 1) * HALF]

    def spot(owner):
        return pl.ds(pl.multiple_of((owner // 2) * 8, 8), 8)

    y_copies = []
    for j in range(1, 8):
        to = lax.rem(sy + j, 8)
        y_copies.append(
            remote(two.at[lax.rem(to, 2), spot(to)], ry.at[j - 1], y_send.at[j - 1], y_recv.at[j - 1], plane[j - 1])
        )
    for copy in y_copies:
        copy.start()
    for copy in y_copies:
        copy.wait_recv()
    side = lax.rem(sy, 2)
    total = two[side, spot(sy), :]
    for j in range(7):
        total = total + ry[j]
    three[side, spot(sy), :] = total
    g_copies = [
        remote(three.at[side, spot(sy)], three.at[side, spot(sy)], g_send.at[j], g_recv.at[j], plane[j])
        for j in range(7)
    ]
    for copy in g_copies:
        copy.start()
    for copy in g_copies:
        copy.wait_recv()
    four[strip(chip), :] = jnp.concatenate([three[0], three[1]], axis=1).astype(BF16)
    w_copies = [
        remote(four.at[strip(chip)], four.at[strip(chip)], w_send.at[j], w_recv.at[j], chips[j]) for j in range(3)
    ]
    for copy in w_copies:
        copy.start()
    for copy in w_copies:
        copy.wait_recv()
    l_copy = remote(four, last, c_send.at[1], c_recv.at[1], mate)
    l_copy.start()
    out[my_half, :] = four[...]
    l_copy.wait_recv()
    out[its_half, :] = last[...]
    for copy in [c_copy, l_copy] + x_copies + y_copies + g_copies + w_copies:
        copy.wait_send()


def combine(part):
    vm = pl.BlockSpec(memory_space=pltpu.VMEM)
    dma = pltpu.SemaphoreType.DMA
    return pl.pallas_call(
        combine_kernel,
        name="combine",
        out_shape=jax.ShapeDtypeStruct((IMAGES, D), BF16),
        in_specs=[vm],
        out_specs=vm,
        scratch_shapes=[
            pltpu.VMEM((128, D), BF16),
            pltpu.VMEM((128, D), BF16),
            pltpu.VMEM((3, 32, D), BF16),
            pltpu.VMEM((2, 32, HALF), F32),
            pltpu.VMEM((7, 8, HALF), F32),
            pltpu.VMEM((2, 32, HALF), F32),
            pltpu.VMEM((128, D), BF16),
            pltpu.VMEM((128, D), BF16),
            dma((2,)),
            dma((2,)),
            dma((3,)),
            dma((3,)),
            dma((7,)),
            dma((7,)),
            dma((7,)),
            dma((7,)),
            dma((3,)),
            dma((3,)),
        ],
        compiler_params=pltpu.CompilerParams(collective_id=1, has_side_effects=True),
    )(part)


def shards(tokens, lengths, ln_gain, w_qkv, w_out):
    rows = tokens.reshape(N, D)
    q, k, v, w_other = gather(rows, ln_gain.reshape(1, D), w_qkv, w_out)
    hidden, part = attend(lengths, q, k, v, rows, w_out, w_other)
    pooled = combine(part).astype(F32)
    return hidden.reshape(1, N, D), pooled.reshape(1, IMAGES, D)


def solution(mesh):
    in_specs = (P("dp", ("sx", "sy"), None), P("dp", None), P(), P("dp", None), P("dp", None))
    out_specs = (P("dp", ("sx", "sy"), None), P("dp", None, None))
    return jax.shard_map(shards, mesh=mesh, in_specs=in_specs, out_specs=out_specs, check_vma=False)
```

```python
import math

import jax
import jax.numpy as jnp
from jax import lax
from jax.experimental import pallas as pl
from jax.experimental.pallas import tpu as pltpu
from jax.sharding import PartitionSpec as P

MESH = pl.DeviceIdType.MESH
F32 = jnp.float32
BF16 = jnp.bfloat16
D = 1280
HALF = 640
N = 512
SIZE = 80
IMAGES = 256
TOTAL = 32768
SCALE = SIZE**-0.5 * math.log2(math.e)
PIECE = 80
UPPER = (0, 1, 2, 6)
CLASSES = (2, 3, 4, 5, 6, 9)
VMEM_LIMIT = 62 * 1024 * 1024


def places():
    sx, sy, d = lax.axis_index("sx"), lax.axis_index("sy"), lax.axis_index("dp")
    h = lax.rem(sy, 2)
    flip = sy + 1 - 2 * h
    shard = sx * 8 + sy
    onward = lax.rem(shard + 2 - 4 * h + 64, 64)
    back = lax.rem(shard - 2 + 4 * h + 64, 64)
    mate = sx + 1 - 2 * lax.rem(sx, 2)
    where = {
        "a": (sx, sy, 1 - d),
        "b": (sx, flip, 1 - d),
        "xp": (lax.rem(sx + 2, 8), sy, d),
        "xm": (lax.rem(sx + 6, 8), sy, d),
        "core": (mate, sy, d),
        "z": (onward // 8, lax.rem(onward, 8), d),
        "zb": (back // 8, lax.rem(back, 8), d),
    }
    return sx, sy, d, h, mate, where


def normalize(rows, gain):
    values = rows.astype(F32)
    center = values - jnp.mean(values, axis=-1, keepdims=True)
    spread = jnp.mean(center * center, axis=-1, keepdims=True)
    return (center * lax.rsqrt(spread + 1e-05) * gain).astype(BF16)


class Exchange:
    def __init__(self, refs, sx, where, send, recv):
        self.refs, self.sx, self.where = refs, sx, where
        self.send, self.recv = send, recv

    def copy(self, kind, c):
        own, other = self.refs[c // 6]
        cols = pl.ds((c % 6) * HALF, HALF)
        upper = c in UPPER
        ahead, src, to = (
            (0, own, "a" if upper else "b"),
            (0, other, "xp"),
            (0, other, "xm"),
            (0, other, "core"),
            (2, other, "xm") if upper else (6, other, "xp"),
            (2, other, "core"),
            (6, other, "core"),
            (4, other, "core"),
        )[kind]
        rows = pl.ds(pl.multiple_of(lax.rem(self.sx + ahead, 8) * PIECE, 16), PIECE)
        return pltpu.make_async_remote_copy(
            src_ref=src.at[rows, cols],
            dst_ref=other.at[rows, cols],
            send_sem=self.send.at[kind * 8 + c],
            recv_sem=self.recv.at[kind * 8 + c],
            device_id=self.where[to],
            device_id_type=MESH,
        )

    def step(self, cs, waits, goes):
        for c in cs:
            for kind in waits:
                self.copy(kind, c).wait_recv()
            for kind in goes:
                self.copy(kind, c).start()

    def begin(self, *cs):
        self.step(cs, (), (0,))

    def from_y(self, *cs):
        self.step(cs, (0,), (1, 2, 3))

    def from_x(self, *cs):
        self.step(cs, (1, 2), (4, 5, 6))

    def from_far(self, *cs):
        self.step(cs, (4,), (7,))

    def finish(self, *cs):
        self.step(cs, (3, 5, 6, 7), ())

    def sent(self):
        for c in range(8):
            for kind in range(8):
                self.copy(kind, c).wait_send()


class Halo:
    def __init__(self, tok, ta, tb, near, far, where, send, recv):
        self.table = []
        for i in range(4):
            self.table += [(tok, i, ta, i, "a"), (tok, 4 + i, tb, i, "b")]
        for i in range(4):
            self.table += [(ta, i, near, i, "b"), (tb, i, near, 4 + i, "a")]
        for i in range(4):
            self.table += [(near, i, far, i, "z"), (near, 4 + i, far, 4 + i, "z")]
        self.where, self.send, self.recv = where, send, recv

    def copy(self, i):
        src, at, dst, to, name = self.table[i]
        return pltpu.make_async_remote_copy(
            src_ref=src.at[pl.ds(64 * at, 64)],
            dst_ref=dst.at[pl.ds(64 * to, 64)],
            send_sem=self.send.at[i],
            recv_sem=self.recv.at[i],
            device_id=self.where[name],
            device_id_type=MESH,
        )

    def own(self, i):
        self.copy(2 * i).start()
        self.copy(2 * i + 1).start()

    def relay(self, i):
        for j in (2 * i, 2 * i + 1):
            self.copy(j).wait_recv()
            self.copy(8 + j).start()

    def onward(self, i):
        for j in (2 * i, 2 * i + 1):
            self.copy(8 + j).wait_recv()
            self.copy(16 + j).start()

    def arrived(self, i):
        for j in (2 * i, 2 * i + 1):
            self.copy(16 + j).wait_recv()

    def sent(self):
        for i in range(24):
            self.copy(i).wait_send()


def gather_kernel(
    tok_hbm, gain_ref, wq_hbm, wo_hbm,
    q_out, k_out, v_out, wo_out,
    tok, wq, wqo, woo, near, far, ta, tb, nrm, nrm2, acc, qs, ks, vs,
    w_send, w_recv, h_send, h_recv, local,
):
    sx, sy, d, h, mate, where = places()
    barrier = pltpu.get_barrier_semaphore()
    for name in ("a", "b", "xp", "xm", "core", "z", "zb"):
        pl.semaphore_signal(barrier, inc=1, device_id=where[name], device_id_type=MESH)

    tok_in = pltpu.make_async_copy(tok_hbm, tok, local.at[0])
    wq_in = pltpu.make_async_copy(wq_hbm, wq, local.at[1])
    tok_in.start()
    wq_in.start()
    pl.semaphore_wait(barrier, 7)

    weights = Exchange(((wq_hbm, wqo), (wo_hbm, woo)), sx, where, w_send, w_recv)
    halo = Halo(tok_hbm, ta, tb, near, far, where, h_send, h_recv)
    gain = gain_ref[...].reshape(1, D)
    mine = pl.ds(pl.multiple_of(d * HALF, 128), HALF)
    others = pl.ds(pl.multiple_of((1 - d) * HALF, 128), HALF)
    near_at = (1 - h) * (2 * N)
    far_at = h * (2 * N)
    outs = []

    def put(src, dst, start, rows, i):
        span = pl.ds(start, rows)
        copy = pltpu.make_async_copy(src.at[span], dst.at[span], local.at[i])
        copy.start()
        outs.append(copy)

    def norm_own(i, _):
        rows = pl.ds(pl.multiple_of(i * 64, 64), 64)
        nrm[rows, :] = normalize(tok[rows, :], gain)
        return 0

    def first_half(part):
        def one(i, _):
            rows = pl.ds(pl.multiple_of(i * 256, 256), 256)
            cols = pl.ds(part * D, D)
            acc[rows, cols] = jnp.dot(nrm[rows, mine], wq[:, cols], preferred_element_type=F32)
            return 0

        lax.fori_loop(0, 2, one, 0)

    def second_half(i, _):
        rows = pl.ds(pl.multiple_of(i * 256, 256), 256)
        into = pl.ds(pl.multiple_of(N + i * 256, 256), 256)
        for part, ref, at, factor in ((0, qs, rows, SCALE), (1, ks, into, None), (2, vs, into, None)):
            cols = pl.ds(part * D, D)
            value = acc[rows, cols] + jnp.dot(nrm[rows, others], wqo[:, cols], preferred_element_type=F32)
            if factor is not None:
                value = value * factor
            ref[at, :] = value.astype(BF16)
        return 0

    def keyvals(src, first, base, slot):
        for j in range(4):
            rows = src[pl.ds(128 * (first + 2 * (j // 2)) + 64 * (j % 2), 64), :]
            nrm2[pl.ds(64 * j, 64), :] = normalize(rows, gain)
        for part, ref, out, sem in ((1, ks, k_out, slot), (2, vs, v_out, slot + 2)):
            cols = pl.ds(part * D, D)
            value = jnp.dot(nrm2[:, mine], wq[:, cols], preferred_element_type=F32)
            value = value + jnp.dot(nrm2[:, others], wqo[:, cols], preferred_element_type=F32)
            for j in range(2):
                start = pl.multiple_of(base + 128 * (first + 2 * j), 128)
                ref[pl.ds(start, 128), :] = value[128 * j : 128 * j + 128].astype(BF16)
                put(ref, out, start, 128, sem + j)

    with jax.named_scope("g0_start"):
        weights.begin(0, 3, 1, 4, 2, 5)
        halo.own(0)
        halo.own(1)
        tok_in.wait()
        lax.fori_loop(0, N // 64, norm_own, 0)
        weights.from_y(0, 3)
        wq_in.wait()
        first_half(0)
        weights.from_y(1, 4)
        first_half(1)
        weights.from_y(2, 5)
        first_half(2)
    with jax.named_scope("g1_relay0"):
        halo.relay(0)
        halo.own(2)
        weights.from_x(0, 3, 1)
    with jax.named_scope("g2_relay1"):
        halo.relay(1)
        weights.begin(6, 7)
        halo.own(3)
        weights.from_x(4, 2, 5)
        halo.onward(0)
    with jax.named_scope("g3_relay2"):
        halo.relay(2)
        halo.onward(1)
        weights.from_far(0, 3, 1, 4, 2, 5)
        halo.relay(3)
    with jax.named_scope("g4_weights"):
        weights.finish(0, 3, 1, 4, 2, 5)
        weights.from_y(6, 7)
    with jax.named_scope("g5_own"):
        lax.fori_loop(0, 2, second_half, 0)
        put(qs, q_out, 0, N, 2)
        put(ks, k_out, N, N, 3)
        put(vs, v_out, N, N, 4)
    with jax.named_scope("g6_near2"):
        halo.onward(2)
        weights.from_x(6, 7)
        keyvals(near, 0, near_at, 5)
    with jax.named_scope("g7_near3"):
        halo.onward(3)
        weights.from_far(6, 7)
        keyvals(near, 1, near_at, 9)
    with jax.named_scope("g8_far1"):
        halo.arrived(0)
        halo.arrived(1)
        keyvals(far, 0, far_at, 13)
        weights.finish(6, 7)
        wo_done = pltpu.make_async_copy(woo, wo_out, local.at[21])
        wo_done.start()
    with jax.named_scope("g9_far3"):
        halo.arrived(2)
        halo.arrived(3)
    with jax.named_scope("g10_end"):
        keyvals(far, 1, far_at, 17)
        for copy in outs:
            copy.wait()
        wo_done.wait()
        weights.sent()
        halo.sent()


def gather(tokens, gain, w_qkv, w_out):
    any_ = pl.BlockSpec(memory_space=pltpu.HBM)
    vm = pl.BlockSpec(memory_space=pltpu.VMEM)
    dma = pltpu.SemaphoreType.DMA
    return pl.pallas_call(
        gather_kernel,
        name="gather",
        out_shape=(
            jax.ShapeDtypeStruct((N, D), BF16),
            jax.ShapeDtypeStruct((3 * N, D), BF16),
            jax.ShapeDtypeStruct((3 * N, D), BF16),
            jax.ShapeDtypeStruct((HALF, D), BF16),
        ),
        in_specs=[any_, vm, any_, any_],
        out_specs=(any_,) * 4,
        scratch_shapes=[
            pltpu.VMEM((N, D), BF16),
            pltpu.VMEM((HALF, 3 * D), BF16),
            pltpu.VMEM((HALF, 3 * D), BF16),
            pltpu.VMEM((HALF, D), BF16),
            pltpu.VMEM((N, D), BF16),
            pltpu.VMEM((N, D), BF16),
            pltpu.VMEM((256, D), BF16),
            pltpu.VMEM((256, D), BF16),
            pltpu.VMEM((N, D), BF16),
            pltpu.VMEM((256, D), BF16),
            pltpu.VMEM((N, 3 * D), F32),
            pltpu.VMEM((N, D), BF16),
            pltpu.VMEM((3 * N, D), BF16),
            pltpu.VMEM((3 * N, D), BF16),
            dma((64,)),
            dma((64,)),
            dma((24,)),
            dma((24,)),
            dma((22,)),
        ],
        compiler_params=pltpu.CompilerParams(
            collective_id=0, has_side_effects=True, vmem_limit_bytes=VMEM_LIMIT
        ),
    )(tokens, gain, w_qkv, w_out)


def attend_kernel(
    lens_ref, q_hbm, k_hbm, v_hbm, tok_hbm, wa_hbm, wb_hbm,
    hid_hbm, part_ref,
    q, k, v, tok, wa, wb, ctx, bias, hid, qid, kid, sems,
):
    sx, sy, d = lax.axis_index("sx"), lax.axis_index("sy"), lax.axis_index("dp")
    copies = [
        pltpu.make_async_copy(a, b, sems.at[i])
        for i, (a, b) in enumerate(
            ((q_hbm, q), (k_hbm, k), (v_hbm, v), (tok_hbm, tok), (wa_hbm, wa), (wb_hbm, wb))
        )
    ]
    for copy in copies:
        copy.start()
    first = (sx * 8 + sy) * N
    base = first - N

    lens = lens_ref[...].astype(F32)
    down = lax.broadcasted_iota(jnp.int32, (IMAGES, IMAGES), 0)
    along = lax.broadcasted_iota(jnp.int32, (IMAGES, IMAGES), 1)
    wide = jnp.broadcast_to(lens, (IMAGES, IMAGES))
    off_col = jnp.sum(jnp.where(along < down, wide, 0.0), axis=1, keepdims=True)
    len_col = jnp.sum(jnp.where(along == down, wide, 0.0), axis=1, keepdims=True)
    off_row = jnp.sum(
        jnp.where(down < along, jnp.broadcast_to(len_col, (IMAGES, IMAGES)), 0.0), axis=0, keepdims=True
    )
    for j in range(3):
        pos = (lax.broadcasted_iota(jnp.int32, (1, N), 1) + (base + j * N)).astype(F32)
        count = jnp.sum(jnp.where(off_col <= pos, 1.0, 0.0), axis=0, keepdims=True) - 1.0
        kid[:, pl.ds(j * N, N)] = jnp.where(pos < TOTAL, count, -1.0)
    for j in range(4):
        pos = (lax.broadcasted_iota(jnp.int32, (128, 1), 0) + (first + j * 128)).astype(F32)
        qid[pl.ds(j * 128, 128), :] = jnp.sum(jnp.where(off_row <= pos, 1.0, 0.0), axis=1, keepdims=True) - 1.0

    for copy in copies[:3]:
        copy.wait()

    def block(i, _):
        rows = pl.ds(pl.multiple_of(i * 128, 128), 128)
        begin = (first + i * 128).astype(F32)
        low = jnp.max(jnp.where(off_row <= begin, off_row, 0.0)).astype(jnp.int32)
        high = jnp.min(jnp.where(off_row > begin + 127.0, off_row, float(TOTAL))).astype(jnp.int32)
        low = (low - base) >> 7
        high = (high - base + 127) >> 7
        blocks = high - low
        ids = qid[rows, :]
        before = 0
        for size in CLASSES:
            n = size * 128

            @pl.when((blocks > before) & (blocks <= size))
            def _():
                start = pl.multiple_of(jnp.minimum(low, 12 - size) * 128, 128)
                keys = pl.ds(start, n)
                bias[:, pl.ds(0, n)] = jnp.where(ids == kid[:, keys], 0.0, -1e30)

                def two_pairs(pp, _):
                    for sub in range(2):
                        pair = pp * 2 + sub
                        tile = (pair * 5) >> 2
                        lanes = pl.ds(pl.multiple_of(tile * 128, 128), 256)
                        shift = pair * 160 - tile * 128
                        lane = lax.broadcasted_iota(jnp.int32, (1, 256), 1) - shift
                        one = (lane >= 0) & (lane < SIZE)
                        two = (lane >= SIZE) & (lane < 2 * SIZE)
                        window = q[rows, lanes]
                        both = jnp.concatenate(
                            [
                                window * jnp.where(one, 1.0, 0.0).astype(BF16),
                                window * jnp.where(two, 1.0, 0.0).astype(BF16),
                            ],
                            axis=0,
                        )
                        scores = lax.dot_general(
                            both, k[keys, lanes], (((1,), (1,)), ((), ())), preferred_element_type=F32
                        )
                        extra = bias[:, pl.ds(0, n)]
                        scores = scores + jnp.concatenate([extra, extra], axis=0)
                        top = jnp.max(scores, axis=1, keepdims=True)
                        weights = jnp.exp2(scores - top)
                        total = jnp.sum(weights, axis=1, keepdims=True)
                        mixed = jnp.dot(weights.astype(BF16), v[keys, lanes], preferred_element_type=F32)
                        mixed = mixed * (1.0 / total)
                        old = ctx[rows, lanes].astype(F32)
                        ctx[rows, lanes] = jnp.where(one, mixed[:128], jnp.where(two, mixed[128:], old)).astype(BF16)
                    return 0

                lax.fori_loop(0, 4, two_pairs, 0)

            before = size
        return 0

    lax.fori_loop(0, 4, block, 0)
    for copy in copies[3:]:
        copy.wait()
    mine = pl.ds(pl.multiple_of(d * HALF, 128), HALF)
    others = pl.ds(pl.multiple_of((1 - d) * HALF, 128), HALF)

    def project(i, _):
        rows = pl.ds(pl.multiple_of(i * 256, 256), 256)
        mixed = jnp.dot(ctx[rows, mine], wa[...], preferred_element_type=F32)
        mixed = mixed + jnp.dot(ctx[rows, others], wb[...], preferred_element_type=F32)
        hid[rows, :] = (tok[rows, :].astype(F32) + mixed).astype(BF16)
        return 0

    lax.fori_loop(0, 2, project, 0)
    out = pltpu.make_async_copy(hid, hid_hbm, sems.at[6])
    out.start()
    image = lax.broadcasted_iota(jnp.int32, (IMAGES, 1), 0).astype(F32)
    onehot = jnp.where(image == kid[:, pl.ds(N, N)], 1.0, 0.0).astype(BF16)
    sums = jnp.dot(onehot, hid[...], preferred_element_type=F32)
    part_ref[...] = (sums / len_col).astype(BF16)
    out.wait()


def attend(lengths, q, k, v, tokens, w_own, w_other):
    any_ = pl.BlockSpec(memory_space=pltpu.HBM)
    vm = pl.BlockSpec(memory_space=pltpu.VMEM)
    return pl.pallas_call(
        attend_kernel,
        name="attend",
        out_shape=(
            jax.ShapeDtypeStruct((N, D), BF16),
            jax.ShapeDtypeStruct((IMAGES, D), BF16),
        ),
        in_specs=[vm] + [any_] * 6,
        out_specs=(any_, vm),
        scratch_shapes=[
            pltpu.VMEM((N, D), BF16),
            pltpu.VMEM((3 * N, D), BF16),
            pltpu.VMEM((3 * N, D), BF16),
            pltpu.VMEM((N, D), BF16),
            pltpu.VMEM((HALF, D), BF16),
            pltpu.VMEM((HALF, D), BF16),
            pltpu.VMEM((N, D), BF16),
            pltpu.VMEM((128, 128 * CLASSES[-1]), F32),
            pltpu.VMEM((N, D), BF16),
            pltpu.VMEM((N, 1), F32),
            pltpu.VMEM((1, 3 * N), F32),
            pltpu.SemaphoreType.DMA((7,)),
        ],
        compiler_params=pltpu.CompilerParams(vmem_limit_bytes=VMEM_LIMIT),
    )(lengths, q, k, v, tokens, w_own, w_other)


def combine_kernel(
    part, out, rc, one, rx, two, ry, three, four, last,
    c_send, c_recv, x_send, x_recv, y_send, y_recv, g_send, g_recv, w_send, w_recv,
):
    sx, sy, d = lax.axis_index("sx"), lax.axis_index("sy"), lax.axis_index("dp")
    core = lax.rem(sx, 2)
    chip = sx // 2
    mate = (sx + 1 - 2 * core, sy, d)
    chips = [(lax.rem(sx + 2 * j, 8), sy, d) for j in (1, 2, 3)]
    plane = [(sx, lax.rem(sy + j, 8), d) for j in range(1, 8)]
    barrier = pltpu.get_barrier_semaphore()
    for who in [mate] + chips + plane:
        pl.semaphore_signal(barrier, inc=1, device_id=who, device_id_type=MESH)
    pl.semaphore_wait(barrier, 11)

    def remote(src, dst, send, recv, who):
        return pltpu.make_async_remote_copy(
            src_ref=src, dst_ref=dst, send_sem=send, recv_sem=recv, device_id=who, device_id_type=MESH
        )

    my_half = pl.ds(pl.multiple_of(core * 128, 128), 128)
    its_half = pl.ds(pl.multiple_of((1 - core) * 128, 128), 128)
    c_copy = remote(part.at[its_half], rc, c_send.at[0], c_recv.at[0], mate)
    c_copy.start()
    c_copy.wait_recv()
    one[...] = (part[my_half, :].astype(F32) + rc[...].astype(F32)).astype(BF16)

    def strip(owner):
        return pl.ds(pl.multiple_of(owner * 32, 32), 32)

    x_copies = [
        remote(one.at[strip(lax.rem(chip + j, 4))], rx.at[j - 1], x_send.at[j - 1], x_recv.at[j - 1], chips[j - 1])
        for j in (1, 2, 3)
    ]
    for copy in x_copies:
        copy.start()
    for copy in x_copies:
        copy.wait_recv()
    total = one[strip(chip), :].astype(F32)
    for j in range(3):
        total = total + rx[j].astype(F32)
    for j in range(2):
        two[j] = total[:, j * HALF : (j + 1) * HALF]

    def spot(owner):
        return pl.ds(pl.multiple_of((owner // 2) * 8, 8), 8)

    y_copies = []
    for j in range(1, 8):
        to = lax.rem(sy + j, 8)
        y_copies.append(
            remote(two.at[lax.rem(to, 2), spot(to)], ry.at[j - 1], y_send.at[j - 1], y_recv.at[j - 1], plane[j - 1])
        )
    for copy in y_copies:
        copy.start()
    for copy in y_copies:
        copy.wait_recv()
    side = lax.rem(sy, 2)
    total = two[side, spot(sy), :]
    for j in range(7):
        total = total + ry[j]
    three[side, spot(sy), :] = total
    g_copies = [
        remote(three.at[side, spot(sy)], three.at[side, spot(sy)], g_send.at[j], g_recv.at[j], plane[j])
        for j in range(7)
    ]
    for copy in g_copies:
        copy.start()
    for copy in g_copies:
        copy.wait_recv()
    four[strip(chip), :] = jnp.concatenate([three[0], three[1]], axis=1).astype(BF16)
    w_copies = [
        remote(four.at[strip(chip)], four.at[strip(chip)], w_send.at[j], w_recv.at[j], chips[j]) for j in range(3)
    ]
    for copy in w_copies:
        copy.start()
    for copy in w_copies:
        copy.wait_recv()
    l_copy = remote(four, last, c_send.at[1], c_recv.at[1], mate)
    l_copy.start()
    out[my_half, :] = four[...].astype(F32)
    l_copy.wait_recv()
    out[its_half, :] = last[...].astype(F32)
    for copy in [c_copy, l_copy] + x_copies + y_copies + g_copies + w_copies:
        copy.wait_send()


def combine(part):
    vm = pl.BlockSpec(memory_space=pltpu.VMEM)
    dma = pltpu.SemaphoreType.DMA
    return pl.pallas_call(
        combine_kernel,
        name="combine",
        out_shape=jax.ShapeDtypeStruct((IMAGES, D), F32),
        in_specs=[vm],
        out_specs=vm,
        scratch_shapes=[
            pltpu.VMEM((128, D), BF16),
            pltpu.VMEM((128, D), BF16),
            pltpu.VMEM((3, 32, D), BF16),
            pltpu.VMEM((2, 32, HALF), F32),
            pltpu.VMEM((7, 8, HALF), F32),
            pltpu.VMEM((2, 32, HALF), F32),
            pltpu.VMEM((128, D), BF16),
            pltpu.VMEM((128, D), BF16),
            dma((2,)),
            dma((2,)),
            dma((3,)),
            dma((3,)),
            dma((7,)),
            dma((7,)),
            dma((7,)),
            dma((7,)),
            dma((3,)),
            dma((3,)),
        ],
        compiler_params=pltpu.CompilerParams(collective_id=1, has_side_effects=True),
    )(part)


def shards(tokens, lengths, ln_gain, w_qkv, w_out):
    rows = tokens.reshape(N, D)
    q, k, v, w_other = gather(rows, ln_gain, w_qkv, w_out)
    hidden, part = attend(lengths, q, k, v, rows, w_out, w_other)
    pooled = combine(part)
    return hidden.reshape(1, N, D), pooled.reshape(1, IMAGES, D)


def solution(mesh):
    in_specs = (P("dp", ("sx", "sy"), None), P("dp", None), P(), P("dp", None), P("dp", None))
    out_specs = (P("dp", ("sx", "sy"), None), P("dp", None, None))
    return jax.shard_map(shards, mesh=mesh, in_specs=in_specs, out_specs=out_specs, check_vma=False)
```

```python
import math

import jax
import jax.numpy as jnp
from jax import lax
from jax.experimental import pallas as pl
from jax.experimental.pallas import tpu as pltpu
from jax.sharding import PartitionSpec as P

MESH = pl.DeviceIdType.MESH
F32 = jnp.float32
BF16 = jnp.bfloat16
D = 1280
HALF = 640
N = 512
SIZE = 80
IMAGES = 256
TOTAL = 32768
SCALE = SIZE**-0.5 * math.log2(math.e)
PIECE = 80
UPPER = (0, 1, 2, 6)
CLASSES = (2, 3, 4, 5, 6, 9)
MIB = 1024 * 1024


def places():
    sx, sy, d = lax.axis_index("sx"), lax.axis_index("sy"), lax.axis_index("dp")
    h = lax.rem(sy, 2)
    flip = sy + 1 - 2 * h
    shard = sx * 8 + sy
    onward = lax.rem(shard + 2 - 4 * h + 64, 64)
    back = lax.rem(shard - 2 + 4 * h + 64, 64)
    mate = sx + 1 - 2 * lax.rem(sx, 2)
    where = {
        "a": (sx, sy, 1 - d),
        "b": (sx, flip, 1 - d),
        "xp": (lax.rem(sx + 2, 8), sy, d),
        "xm": (lax.rem(sx + 6, 8), sy, d),
        "core": (mate, sy, d),
        "z": (onward // 8, lax.rem(onward, 8), d),
        "zb": (back // 8, lax.rem(back, 8), d),
    }
    return sx, sy, d, h, mate, where


def normalize(rows, gain):
    values = rows.astype(F32)
    center = values - jnp.mean(values, axis=-1, keepdims=True)
    spread = jnp.mean(center * center, axis=-1, keepdims=True)
    return (center * lax.rsqrt(spread + 1e-05) * gain).astype(BF16)


class Exchange:
    def __init__(self, refs, sx, where, send, recv):
        self.refs, self.sx, self.where = refs, sx, where
        self.send, self.recv = send, recv

    def copy(self, kind, c):
        own, other = self.refs[c // 6]
        cols = pl.ds((c % 6) * HALF, HALF)
        upper = c in UPPER
        ahead, src, to = (
            (0, own, "a" if upper else "b"),
            (0, other, "xp"),
            (0, other, "xm"),
            (0, other, "core"),
            (2, other, "xm") if upper else (6, other, "xp"),
            (2, other, "core"),
            (6, other, "core"),
            (4, other, "core"),
        )[kind]
        rows = pl.ds(pl.multiple_of(lax.rem(self.sx + ahead, 8) * PIECE, 16), PIECE)
        return pltpu.make_async_remote_copy(
            src_ref=src.at[rows, cols],
            dst_ref=other.at[rows, cols],
            send_sem=self.send.at[kind * 8 + c],
            recv_sem=self.recv.at[kind * 8 + c],
            device_id=self.where[to],
            device_id_type=MESH,
        )

    def step(self, cs, waits, goes):
        for c in cs:
            for kind in waits:
                self.copy(kind, c).wait_recv()
            for kind in goes:
                self.copy(kind, c).start()

    def begin(self, *cs):
        self.step(cs, (), (0,))

    def from_y(self, *cs):
        self.step(cs, (0,), (1, 2, 3))

    def from_x(self, *cs):
        self.step(cs, (1, 2), (4, 5, 6))

    def from_far(self, *cs):
        self.step(cs, (4,), (7,))

    def finish(self, *cs):
        self.step(cs, (3, 5, 6, 7), ())

    def sent(self):
        for c in range(8):
            for kind in range(8):
                self.copy(kind, c).wait_send()


class Halo:
    def __init__(self, tok, ta, tb, near, far, where, send, recv):
        self.table = []
        for i in range(4):
            self.table += [(tok, i, ta, i, "a"), (tok, 4 + i, tb, i, "b")]
        for i in range(4):
            self.table += [(ta, i, near, i, "b"), (tb, i, near, 4 + i, "a")]
        for i in range(4):
            self.table += [(near, i, far, i, "z"), (near, 4 + i, far, 4 + i, "z")]
        self.where, self.send, self.recv = where, send, recv

    def copy(self, i):
        src, at, dst, to, name = self.table[i]
        return pltpu.make_async_remote_copy(
            src_ref=src.at[pl.ds(64 * at, 64)],
            dst_ref=dst.at[pl.ds(64 * to, 64)],
            send_sem=self.send.at[i],
            recv_sem=self.recv.at[i],
            device_id=self.where[name],
            device_id_type=MESH,
        )

    def own(self, i):
        self.copy(2 * i).start()
        self.copy(2 * i + 1).start()

    def relay(self, i):
        for j in (2 * i, 2 * i + 1):
            self.copy(j).wait_recv()
            self.copy(8 + j).start()

    def onward(self, i):
        for j in (2 * i, 2 * i + 1):
            self.copy(8 + j).wait_recv()
            self.copy(16 + j).start()

    def arrived(self, i):
        for j in (2 * i, 2 * i + 1):
            self.copy(16 + j).wait_recv()

    def sent(self):
        for i in range(24):
            self.copy(i).wait_send()


def gather_kernel(
    tok_hbm, gain_ref, wq_hbm, wo_hbm,
    qs, ks, vs, woo,
    tok, wq, wqo, near, far, ta, tb, nrm, nrm2, acc,
    w_send, w_recv, h_send, h_recv, local,
):
    sx, sy, d, h, mate, where = places()
    barrier = pltpu.get_barrier_semaphore()
    for name in ("a", "b", "xp", "xm", "core", "z", "zb"):
        pl.semaphore_signal(barrier, inc=1, device_id=where[name], device_id_type=MESH)

    tok_in = pltpu.make_async_copy(tok_hbm, tok, local.at[0])
    wq_in = pltpu.make_async_copy(wq_hbm, wq, local.at[1])
    tok_in.start()
    wq_in.start()
    pl.semaphore_wait(barrier, 7)

    weights = Exchange(((wq_hbm, wqo), (wo_hbm, woo)), sx, where, w_send, w_recv)
    halo = Halo(tok_hbm, ta, tb, near, far, where, h_send, h_recv)
    gain = gain_ref[...].reshape(1, D)
    mine = pl.ds(pl.multiple_of(d * HALF, 128), HALF)
    others = pl.ds(pl.multiple_of((1 - d) * HALF, 128), HALF)
    near_at = (1 - h) * (2 * N)
    far_at = h * (2 * N)

    def norm_own(i, _):
        rows = pl.ds(pl.multiple_of(i * 64, 64), 64)
        nrm[rows, :] = normalize(tok[rows, :], gain)
        return 0

    def first_half(part):
        def one(i, _):
            rows = pl.ds(pl.multiple_of(i * 256, 256), 256)
            cols = pl.ds(part * D, D)
            acc[rows, cols] = jnp.dot(nrm[rows, mine], wq[:, cols], preferred_element_type=F32)
            return 0

        lax.fori_loop(0, 2, one, 0)

    def second_half(i, _):
        rows = pl.ds(pl.multiple_of(i * 256, 256), 256)
        into = pl.ds(pl.multiple_of(N + i * 256, 256), 256)
        for part, ref, at, factor in ((0, qs, rows, SCALE), (1, ks, into, None), (2, vs, into, None)):
            cols = pl.ds(part * D, D)
            value = acc[rows, cols] + jnp.dot(nrm[rows, others], wqo[:, cols], preferred_element_type=F32)
            if factor is not None:
                value = value * factor
            ref[at, :] = value.astype(BF16)
        return 0

    def keyvals(src, first, base):
        for j in range(4):
            rows = src[pl.ds(128 * (first + 2 * (j // 2)) + 64 * (j % 2), 64), :]
            nrm2[pl.ds(64 * j, 64), :] = normalize(rows, gain)
        for part, ref in ((1, ks), (2, vs)):
            cols = pl.ds(part * D, D)
            value = jnp.dot(nrm2[:, mine], wq[:, cols], preferred_element_type=F32)
            value = value + jnp.dot(nrm2[:, others], wqo[:, cols], preferred_element_type=F32)
            for j in range(2):
                start = pl.multiple_of(base + 128 * (first + 2 * j), 128)
                ref[pl.ds(start, 128), :] = value[128 * j : 128 * j + 128].astype(BF16)

    with jax.named_scope("g0_start"):
        weights.begin(0, 3, 1, 4, 2, 5)
        halo.own(0)
        halo.own(1)
        tok_in.wait()
        lax.fori_loop(0, N // 64, norm_own, 0)
        weights.from_y(0, 3)
        wq_in.wait()
        first_half(0)
        weights.from_y(1, 4)
        first_half(1)
        weights.from_y(2, 5)
        first_half(2)
    with jax.named_scope("g1_relay0"):
        halo.relay(0)
        halo.own(2)
        weights.from_x(0, 3, 1)
    with jax.named_scope("g2_relay1"):
        halo.relay(1)
        weights.begin(6, 7)
        halo.own(3)
        weights.from_x(4, 2, 5)
        halo.onward(0)
    with jax.named_scope("g3_relay2"):
        halo.relay(2)
        halo.onward(1)
        weights.from_far(0, 3, 1, 4, 2, 5)
        halo.relay(3)
    with jax.named_scope("g4_weights"):
        weights.finish(0, 3, 1, 4, 2, 5)
        weights.from_y(6, 7)
    with jax.named_scope("g5_own"):
        lax.fori_loop(0, 2, second_half, 0)
    with jax.named_scope("g6_near2"):
        halo.onward(2)
        weights.from_x(6, 7)
        keyvals(near, 0, near_at)
    with jax.named_scope("g7_near3"):
        halo.onward(3)
        weights.from_far(6, 7)
        keyvals(near, 1, near_at)
    with jax.named_scope("g8_far1"):
        halo.arrived(0)
        halo.arrived(1)
        keyvals(far, 0, far_at)
        weights.finish(6, 7)
    with jax.named_scope("g9_far3"):
        halo.arrived(2)
        halo.arrived(3)
    with jax.named_scope("g10_end"):
        keyvals(far, 1, far_at)
        weights.sent()
        halo.sent()


def held(x):
    return pltpu.with_memory_space_constraint(x, pltpu.VMEM)


def outside(x):
    return pltpu.with_memory_space_constraint(x, pltpu.HBM)


def gather(tokens, gain, w_qkv, w_out):
    any_ = pl.BlockSpec(memory_space=pltpu.HBM)
    vm = pl.BlockSpec(memory_space=pltpu.VMEM)
    dma = pltpu.SemaphoreType.DMA
    return pl.pallas_call(
        gather_kernel,
        name="gather",
        out_shape=(
            pltpu.VMEM((N, D), BF16),
            pltpu.VMEM((3 * N, D), BF16),
            pltpu.VMEM((3 * N, D), BF16),
            pltpu.VMEM((HALF, D), BF16),
        ),
        in_specs=[any_, vm, any_, any_],
        out_specs=(vm,) * 4,
        scratch_shapes=[
            pltpu.VMEM((N, D), BF16),
            pltpu.VMEM((HALF, 3 * D), BF16),
            pltpu.VMEM((HALF, 3 * D), BF16),
            pltpu.VMEM((N, D), BF16),
            pltpu.VMEM((N, D), BF16),
            pltpu.VMEM((256, D), BF16),
            pltpu.VMEM((256, D), BF16),
            pltpu.VMEM((N, D), BF16),
            pltpu.VMEM((256, D), BF16),
            pltpu.VMEM((N, 3 * D), F32),
            dma((64,)),
            dma((64,)),
            dma((24,)),
            dma((24,)),
            dma((2,)),
        ],
        compiler_params=pltpu.CompilerParams(
            collective_id=0, has_side_effects=True, vmem_limit_bytes=40 * MIB
        ),
    )(outside(tokens), gain, outside(w_qkv), outside(w_out))


def attend_kernel(
    lens_ref, q, k, v, wb, tok_hbm, wa_hbm,
    hid_hbm, part_ref,
    tok, wa, ctx, bias, hid, qid, kid, sems,
):
    sx, sy, d = lax.axis_index("sx"), lax.axis_index("sy"), lax.axis_index("dp")
    copies = [
        pltpu.make_async_copy(a, b, sems.at[i])
        for i, (a, b) in enumerate(
            ((tok_hbm, tok), (wa_hbm, wa))
        )
    ]
    for copy in copies:
        copy.start()
    first = (sx * 8 + sy) * N
    base = first - N

    lens = lens_ref[...].astype(F32)
    down = lax.broadcasted_iota(jnp.int32, (IMAGES, IMAGES), 0)
    along = lax.broadcasted_iota(jnp.int32, (IMAGES, IMAGES), 1)
    wide = jnp.broadcast_to(lens, (IMAGES, IMAGES))
    off_col = jnp.sum(jnp.where(along < down, wide, 0.0), axis=1, keepdims=True)
    len_col = jnp.sum(jnp.where(along == down, wide, 0.0), axis=1, keepdims=True)
    off_row = jnp.sum(
        jnp.where(down < along, jnp.broadcast_to(len_col, (IMAGES, IMAGES)), 0.0), axis=0, keepdims=True
    )
    for j in range(3):
        pos = (lax.broadcasted_iota(jnp.int32, (1, N), 1) + (base + j * N)).astype(F32)
        count = jnp.sum(jnp.where(off_col <= pos, 1.0, 0.0), axis=0, keepdims=True) - 1.0
        kid[:, pl.ds(j * N, N)] = jnp.where(pos < TOTAL, count, -1.0)
    for j in range(4):
        pos = (lax.broadcasted_iota(jnp.int32, (128, 1), 0) + (first + j * 128)).astype(F32)
        qid[pl.ds(j * 128, 128), :] = jnp.sum(jnp.where(off_row <= pos, 1.0, 0.0), axis=1, keepdims=True) - 1.0

    def block(i, _):
        rows = pl.ds(pl.multiple_of(i * 128, 128), 128)
        begin = (first + i * 128).astype(F32)
        low = jnp.max(jnp.where(off_row <= begin, off_row, 0.0)).astype(jnp.int32)
        high = jnp.min(jnp.where(off_row > begin + 127.0, off_row, float(TOTAL))).astype(jnp.int32)
        low = (low - base) >> 7
        high = (high - base + 127) >> 7
        blocks = high - low
        ids = qid[rows, :]
        before = 0
        for size in CLASSES:
            n = size * 128

            @pl.when((blocks > before) & (blocks <= size))
            def _():
                start = pl.multiple_of(jnp.minimum(low, 12 - size) * 128, 128)
                keys = pl.ds(start, n)
                bias[:, pl.ds(0, n)] = jnp.where(ids == kid[:, keys], 0.0, -1e30)

                def two_pairs(pp, _):
                    for sub in range(2):
                        pair = pp * 2 + sub
                        tile = (pair * 5) >> 2
                        lanes = pl.ds(pl.multiple_of(tile * 128, 128), 256)
                        shift = pair * 160 - tile * 128
                        lane = lax.broadcasted_iota(jnp.int32, (1, 256), 1) - shift
                        one = (lane >= 0) & (lane < SIZE)
                        two = (lane >= SIZE) & (lane < 2 * SIZE)
                        window = q[rows, lanes]
                        both = jnp.concatenate(
                            [
                                window * jnp.where(one, 1.0, 0.0).astype(BF16),
                                window * jnp.where(two, 1.0, 0.0).astype(BF16),
                            ],
                            axis=0,
                        )
                        scores = lax.dot_general(
                            both, k[keys, lanes], (((1,), (1,)), ((), ())), preferred_element_type=F32
                        )
                        extra = bias[:, pl.ds(0, n)]
                        scores = scores + jnp.concatenate([extra, extra], axis=0)
                        top = jnp.max(scores, axis=1, keepdims=True)
                        weights = jnp.exp2(scores - top)
                        total = jnp.sum(weights, axis=1, keepdims=True)
                        mixed = jnp.dot(weights.astype(BF16), v[keys, lanes], preferred_element_type=F32)
                        mixed = mixed * (1.0 / total)
                        old = ctx[rows, lanes].astype(F32)
                        ctx[rows, lanes] = jnp.where(one, mixed[:128], jnp.where(two, mixed[128:], old)).astype(BF16)
                    return 0

                lax.fori_loop(0, 4, two_pairs, 0)

            before = size
        return 0

    lax.fori_loop(0, 4, block, 0)
    for copy in copies:
        copy.wait()
    mine = pl.ds(pl.multiple_of(d * HALF, 128), HALF)
    others = pl.ds(pl.multiple_of((1 - d) * HALF, 128), HALF)

    def project(i, _):
        rows = pl.ds(pl.multiple_of(i * 256, 256), 256)
        mixed = jnp.dot(ctx[rows, mine], wa[...], preferred_element_type=F32)
        mixed = mixed + jnp.dot(ctx[rows, others], wb[...], preferred_element_type=F32)
        hid[rows, :] = (tok[rows, :].astype(F32) + mixed).astype(BF16)
        return 0

    lax.fori_loop(0, 2, project, 0)
    out = pltpu.make_async_copy(hid, hid_hbm, sems.at[2])
    out.start()
    image = lax.broadcasted_iota(jnp.int32, (IMAGES, 1), 0).astype(F32)
    onehot = jnp.where(image == kid[:, pl.ds(N, N)], 1.0, 0.0).astype(BF16)
    sums = jnp.dot(onehot, hid[...], preferred_element_type=F32)
    part_ref[...] = (sums / len_col).astype(BF16)
    out.wait()


def attend(lengths, q, k, v, w_other, tokens, w_own):
    any_ = pl.BlockSpec(memory_space=pltpu.HBM)
    vm = pl.BlockSpec(memory_space=pltpu.VMEM)
    return pl.pallas_call(
        attend_kernel,
        name="attend",
        out_shape=(
            jax.ShapeDtypeStruct((N, D), BF16),
            pltpu.VMEM((IMAGES, D), BF16),
        ),
        in_specs=[vm] * 5 + [any_] * 2,
        out_specs=(any_, vm),
        scratch_shapes=[
            pltpu.VMEM((N, D), BF16),
            pltpu.VMEM((HALF, D), BF16),
            pltpu.VMEM((N, D), BF16),
            pltpu.VMEM((128, 128 * CLASSES[-1]), F32),
            pltpu.VMEM((N, D), BF16),
            pltpu.VMEM((N, 1), F32),
            pltpu.VMEM((1, 3 * N), F32),
            pltpu.SemaphoreType.DMA((3,)),
        ],
        compiler_params=pltpu.CompilerParams(vmem_limit_bytes=28 * MIB),
    )(lengths, *[held(x) for x in (q, k, v, w_other)], outside(tokens), outside(w_own))


def combine_kernel(
    part, out, rc, one, rx, two, ry, three, four, last,
    c_send, c_recv, x_send, x_recv, y_send, y_recv, g_send, g_recv, w_send, w_recv,
):
    sx, sy, d = lax.axis_index("sx"), lax.axis_index("sy"), lax.axis_index("dp")
    core = lax.rem(sx, 2)
    chip = sx // 2
    mate = (sx + 1 - 2 * core, sy, d)
    chips = [(lax.rem(sx + 2 * j, 8), sy, d) for j in (1, 2, 3)]
    plane = [(sx, lax.rem(sy + j, 8), d) for j in range(1, 8)]
    barrier = pltpu.get_barrier_semaphore()
    for who in [mate] + chips + plane:
        pl.semaphore_signal(barrier, inc=1, device_id=who, device_id_type=MESH)
    pl.semaphore_wait(barrier, 11)

    def remote(src, dst, send, recv, who):
        return pltpu.make_async_remote_copy(
            src_ref=src, dst_ref=dst, send_sem=send, recv_sem=recv, device_id=who, device_id_type=MESH
        )

    my_half = pl.ds(pl.multiple_of(core * 128, 128), 128)
    its_half = pl.ds(pl.multiple_of((1 - core) * 128, 128), 128)
    c_copy = remote(part.at[its_half], rc, c_send.at[0], c_recv.at[0], mate)
    c_copy.start()
    c_copy.wait_recv()
    one[...] = (part[my_half, :].astype(F32) + rc[...].astype(F32)).astype(BF16)

    def strip(owner):
        return pl.ds(pl.multiple_of(owner * 32, 32), 32)

    x_copies = [
        remote(one.at[strip(lax.rem(chip + j, 4))], rx.at[j - 1], x_send.at[j - 1], x_recv.at[j - 1], chips[j - 1])
        for j in (1, 2, 3)
    ]
    for copy in x_copies:
        copy.start()
    for copy in x_copies:
        copy.wait_recv()
    total = one[strip(chip), :].astype(F32)
    for j in range(3):
        total = total + rx[j].astype(F32)
    for j in range(2):
        two[j] = total[:, j * HALF : (j + 1) * HALF]

    def spot(owner):
        return pl.ds(pl.multiple_of((owner // 2) * 8, 8), 8)

    y_copies = []
    for j in range(1, 8):
        to = lax.rem(sy + j, 8)
        y_copies.append(
            remote(two.at[lax.rem(to, 2), spot(to)], ry.at[j - 1], y_send.at[j - 1], y_recv.at[j - 1], plane[j - 1])
        )
    for copy in y_copies:
        copy.start()
    for copy in y_copies:
        copy.wait_recv()
    side = lax.rem(sy, 2)
    total = two[side, spot(sy), :]
    for j in range(7):
        total = total + ry[j]
    three[side, spot(sy), :] = total
    g_copies = [
        remote(three.at[side, spot(sy)], three.at[side, spot(sy)], g_send.at[j], g_recv.at[j], plane[j])
        for j in range(7)
    ]
    for copy in g_copies:
        copy.start()
    for copy in g_copies:
        copy.wait_recv()
    four[strip(chip), :] = jnp.concatenate([three[0], three[1]], axis=1).astype(BF16)
    w_copies = [
        remote(four.at[strip(chip)], four.at[strip(chip)], w_send.at[j], w_recv.at[j], chips[j]) for j in range(3)
    ]
    for copy in w_copies:
        copy.start()
    for copy in w_copies:
        copy.wait_recv()
    l_copy = remote(four, last, c_send.at[1], c_recv.at[1], mate)
    l_copy.start()
    out[my_half, :] = four[...].astype(F32)
    l_copy.wait_recv()
    out[its_half, :] = last[...].astype(F32)
    for copy in [c_copy, l_copy] + x_copies + y_copies + g_copies + w_copies:
        copy.wait_send()


def combine(part):
    vm = pl.BlockSpec(memory_space=pltpu.VMEM)
    dma = pltpu.SemaphoreType.DMA
    return pl.pallas_call(
        combine_kernel,
        name="combine",
        out_shape=pltpu.VMEM((IMAGES, D), F32),
        in_specs=[vm],
        out_specs=vm,
        scratch_shapes=[
            pltpu.VMEM((128, D), BF16),
            pltpu.VMEM((128, D), BF16),
            pltpu.VMEM((3, 32, D), BF16),
            pltpu.VMEM((2, 32, HALF), F32),
            pltpu.VMEM((7, 8, HALF), F32),
            pltpu.VMEM((2, 32, HALF), F32),
            pltpu.VMEM((128, D), BF16),
            pltpu.VMEM((128, D), BF16),
            dma((2,)),
            dma((2,)),
            dma((3,)),
            dma((3,)),
            dma((7,)),
            dma((7,)),
            dma((7,)),
            dma((7,)),
            dma((3,)),
            dma((3,)),
        ],
        compiler_params=pltpu.CompilerParams(
            collective_id=1, has_side_effects=True, vmem_limit_bytes=8 * MIB
        ),
    )(held(part))


def shards(tokens, lengths, ln_gain, w_qkv, w_out):
    rows = tokens.reshape(N, D)
    q, k, v, w_other = gather(rows, ln_gain, w_qkv, w_out)
    hidden, part = attend(lengths, q, k, v, w_other, rows, w_out)
    pooled = combine(part)
    return hidden.reshape(1, N, D), pooled.reshape(1, IMAGES, D)


def solution(mesh):
    in_specs = (P("dp", ("sx", "sy"), None), P("dp", None), P(), P("dp", None), P("dp", None))
    out_specs = (P("dp", ("sx", "sy"), None), P("dp", None, None))
    return jax.shard_map(shards, mesh=mesh, in_specs=in_specs, out_specs=out_specs, check_vma=False)
```

```python
import math

import jax
import jax.numpy as jnp
from jax import lax
from jax.experimental import pallas as pl
from jax.experimental.pallas import tpu as pltpu
from jax.sharding import PartitionSpec as P

MESH = pl.DeviceIdType.MESH
F32 = jnp.float32
BF16 = jnp.bfloat16
D = 1280
HALF = 640
N = 512
SIZE = 80
IMAGES = 256
TOTAL = 32768
SCALE = SIZE**-0.5 * math.log2(math.e)
PIECE = 80
CLASSES = (2, 3, 4, 5, 6, 9)
MIB = 1024 * 1024


def places():
    sx, sy, d = lax.axis_index("sx"), lax.axis_index("sy"), lax.axis_index("dp")
    h = lax.rem(sy, 2)
    flip = sy + 1 - 2 * h
    shard = sx * 8 + sy
    onward = lax.rem(shard + 2 - 4 * h + 64, 64)
    back = lax.rem(shard - 2 + 4 * h + 64, 64)
    mate = sx + 1 - 2 * lax.rem(sx, 2)
    where = {
        "a": (sx, sy, 1 - d),
        "b": (sx, flip, 1 - d),
        "xp": (lax.rem(sx + 2, 8), sy, d),
        "xm": (lax.rem(sx + 6, 8), sy, d),
        "core": (mate, sy, d),
        "z": (onward // 8, lax.rem(onward, 8), d),
        "zb": (back // 8, lax.rem(back, 8), d),
        "zi": (sx, lax.rem(sy + 6 + 4 * h, 8), d),
        "zj": (sx, lax.rem(sy + 10 - 4 * h, 8), d),
    }
    z = sy // 2
    first, last = (3 - z) // 3, z // 3
    where["hop"] = (6 - 4 * h * first, 2 + 4 * (1 - h) * last)
    return sx, sy, d, h, mate, where


def normalize(rows, gain):
    values = rows.astype(F32)
    center = values - jnp.mean(values, axis=-1, keepdims=True)
    spread = jnp.mean(center * center, axis=-1, keepdims=True)
    return (center * lax.rsqrt(spread + 1e-05) * gain).astype(BF16)


class Exchange:
    def __init__(self, own, other, sx, z, turn, where, send, recv):
        self.own, self.other, self.sx, self.z, self.turn = own, other, sx, z, turn
        self.where, self.send, self.recv = where, send, recv

    def copy(self, kind, t, side):
        pair = lax.rem(self.z + self.turn * (t - (kind == 8)) + 8, 4)
        chunk = pair + 3 + pair // 3 if side else pair + 3 * (pair // 3)
        cols = pl.ds(pl.multiple_of(chunk * HALF, 128), HALF)
        own, other, where = self.own, self.other, self.where
        hop = where["hop"][side] if t else (6, 2)[side]
        ahead, src, to = (
            (0, own, where["b" if side else "a"]),
            (0, other, where["xp"]),
            (0, other, where["xm"]),
            (0, other, where["core"]),
            (8 - hop, other, (lax.rem(self.sx + hop, 8),) + where["core"][1:]),
            (2, other, where["core"]),
            (6, other, where["core"]),
            (4, other, where["core"]),
            (0, other, where["zi"]),
        )[kind]
        rows = pl.ds(pl.multiple_of(lax.rem(self.sx + ahead, 8) * PIECE, 16), PIECE)
        i = kind * 8 + side * 4 + t
        return pltpu.make_async_remote_copy(
            src_ref=src.at[rows, cols],
            dst_ref=other.at[rows, cols],
            send_sem=self.send.at[i],
            recv_sem=self.recv.at[i],
            device_id=to,
            device_id_type=MESH,
        )

    def begin(self):
        for side in range(2):
            self.copy(0, 0, side).start()

    def landed(self, t):
        for side in range(2):
            self.copy(8 if t else 0, t, side).wait_recv()
            if t < 3:
                self.copy(8, t + 1, side).start()
            for kind in (1, 2, 3):
                self.copy(kind, t, side).start()

    def from_x(self, t):
        for side in range(2):
            for kind in (1, 2):
                self.copy(kind, t, side).wait_recv()
            for kind in (4, 5, 6):
                self.copy(kind, t, side).start()

    def from_far(self, t):
        for side in range(2):
            self.copy(4, t, side).wait_recv()
            self.copy(7, t, side).start()

    def finish(self):
        for t in range(4):
            for side in range(2):
                for kind in (3, 5, 6, 7):
                    self.copy(kind, t, side).wait_recv()

    def sent(self):
        for side in range(2):
            for t in range(4):
                for kind in range(1, 8):
                    self.copy(kind, t, side).wait_send()
                self.copy(8 if t else 0, t, side).wait_send()


class Halo:
    def __init__(self, tok, ta, tb, near, far, where, send, recv):
        self.table = []
        for i in range(4):
            self.table += [(tok, i, ta, i, "a"), (tok, 4 + i, tb, i, "b")]
        for i in range(4):
            self.table += [(ta, i, near, i, "b"), (tb, i, near, 4 + i, "a")]
        for i in range(4):
            self.table += [(near, i, far, i, "z"), (near, 4 + i, far, 4 + i, "z")]
        self.where, self.send, self.recv = where, send, recv

    def copy(self, i):
        src, at, dst, to, name = self.table[i]
        return pltpu.make_async_remote_copy(
            src_ref=src.at[pl.ds(64 * at, 64)],
            dst_ref=dst.at[pl.ds(64 * to, 64)],
            send_sem=self.send.at[i],
            recv_sem=self.recv.at[i],
            device_id=self.where[name],
            device_id_type=MESH,
        )

    def own(self, i):
        self.copy(2 * i).start()
        self.copy(2 * i + 1).start()

    def relay(self, i):
        for j in (2 * i, 2 * i + 1):
            self.copy(j).wait_recv()
            self.copy(8 + j).start()

    def onward(self, i):
        for j in (2 * i, 2 * i + 1):
            self.copy(8 + j).wait_recv()
            self.copy(16 + j).start()

    def arrived(self, i):
        for j in (2 * i, 2 * i + 1):
            self.copy(16 + j).wait_recv()

    def sent(self):
        for i in range(24):
            self.copy(i).wait_send()


def gather_kernel(
    tok_hbm, gain_ref, wq_hbm, wo_hbm,
    qs, ks, vs, wall,
    tok, wown, near, far, ta, tb, nrm, nrmh, acc, acch,
    w_send, w_recv, h_send, h_recv, local,
):
    sx, sy, d, h, mate, where = places()
    wq_in = pltpu.make_async_copy(wq_hbm, wown.at[:, pl.ds(0, 3 * D)], local.at[1])
    wo_in = pltpu.make_async_copy(wo_hbm, wown.at[:, pl.ds(3 * D, D)], local.at[2])
    tok_in = pltpu.make_async_copy(tok_hbm, tok, local.at[0])
    wq_in.start()
    wo_in.start()
    tok_in.start()
    barrier = pltpu.get_barrier_semaphore()
    partners = ("a", "b", "xp", "xm", "core", "z", "zb", "zi", "zj")
    for name in partners:
        pl.semaphore_signal(barrier, inc=1, device_id=where[name], device_id_type=MESH)
    wq_in.wait()
    wo_in.wait()
    pl.semaphore_wait(barrier, len(partners))

    weights = Exchange(wown, wall, sx, sy // 2, 1 - 2 * h, where, w_send, w_recv)
    halo = Halo(tok_hbm, ta, tb, near, far, where, h_send, h_recv)
    gain = gain_ref[...].reshape(1, D)
    mine = pl.ds(pl.multiple_of(d * HALF, 128), HALF)
    others = pl.ds(pl.multiple_of((1 - d) * HALF, 128), HALF)
    near_at = (1 - h) * (2 * N)
    far_at = h * (2 * N)

    def norm_own(i, _):
        rows = pl.ds(pl.multiple_of(i * 64, 64), 64)
        nrm[rows, :] = normalize(tok[rows, :], gain)
        return 0

    def first_half(part):
        def one(i, _):
            rows = pl.ds(pl.multiple_of(i * 256, 256), 256)
            cols = pl.ds(part * D, D)
            acc[rows, cols] = jnp.dot(nrm[rows, mine], wown[:, cols], preferred_element_type=F32)
            return 0

        lax.fori_loop(0, 2, one, 0)

    def second_half(i, _):
        rows = pl.ds(pl.multiple_of(i * 256, 256), 256)
        into = pl.ds(pl.multiple_of(N + i * 256, 256), 256)
        for part, ref, at, factor in ((0, qs, rows, SCALE), (1, ks, into, None), (2, vs, into, None)):
            cols = pl.ds(part * D, D)
            value = acc[rows, cols] + jnp.dot(nrm[rows, others], wall[:, cols], preferred_element_type=F32)
            if factor is not None:
                value = value * factor
            ref[at, :] = value.astype(BF16)
        return 0

    def halo_first(src, first, group):
        def one(j, _):
            at = pl.multiple_of(128 * first + 64 * lax.rem(j, 2) + 256 * (j // 2), 64)
            to = pl.multiple_of(256 * group + 64 * j, 64)
            nrmh[pl.ds(to, 64), :] = normalize(src[pl.ds(at, 64), :], gain)
            return 0

        lax.fori_loop(0, 4, one, 0)
        rows = pl.ds(256 * group, 256)
        for part in range(2):
            acch[rows, pl.ds(part * D, D)] = jnp.dot(
                nrmh[rows, mine], wown[:, pl.ds((part + 1) * D, D)], preferred_element_type=F32
            )

    def halo_second(first, base, group):
        rows = pl.ds(256 * group, 256)
        for part, ref in ((0, ks), (1, vs)):
            value = acch[rows, pl.ds(part * D, D)] + jnp.dot(
                nrmh[rows, others], wall[:, pl.ds((part + 1) * D, D)], preferred_element_type=F32
            )
            for j in range(2):
                start = pl.multiple_of(base + 128 * first + 256 * j, 128)
                ref[pl.ds(start, 128), :] = value[128 * j : 128 * j + 128].astype(BF16)

    with jax.named_scope("g0"):
        weights.begin()
        halo.own(0)
        halo.own(1)
        tok_in.wait()
        lax.fori_loop(0, N // 64, norm_own, 0)
        weights.landed(0)
        first_half(0)
    with jax.named_scope("g1"):
        halo.relay(0)
        halo.own(2)
        first_half(1)
        weights.landed(1)
    with jax.named_scope("g2"):
        halo.relay(1)
        halo.own(3)
        first_half(2)
        weights.landed(2)
    with jax.named_scope("g3"):
        halo.onward(0)
        weights.from_x(0)
        weights.landed(3)
    with jax.named_scope("g4"):
        halo.relay(2)
        weights.from_x(1)
        halo.onward(1)
        weights.from_x(2)
    with jax.named_scope("g5"):
        halo_first(near, 0, 0)
        halo.relay(3)
    with jax.named_scope("g6"):
        weights.from_far(0)
        weights.from_x(3)
        halo.onward(2)
        weights.from_far(1)
        halo.onward(3)
    with jax.named_scope("g7"):
        weights.from_far(2)
        halo_first(near, 1, 1)
    with jax.named_scope("g8"):
        weights.from_far(3)
        halo.arrived(0)
        halo.arrived(1)
        halo_first(far, 0, 2)
        weights.finish()
    with jax.named_scope("g9"):
        lax.fori_loop(0, 2, second_half, 0)
        halo_second(0, near_at, 0)
        halo_second(1, near_at, 1)
        halo_second(0, far_at, 2)
    with jax.named_scope("g12"):
        halo.arrived(2)
        halo.arrived(3)
    with jax.named_scope("g13"):
        halo_first(far, 1, 0)
        halo_second(1, far_at, 0)
        weights.sent()
        halo.sent()


def held(x):
    return pltpu.with_memory_space_constraint(x, pltpu.VMEM)


def outside(x):
    return pltpu.with_memory_space_constraint(x, pltpu.HBM)


def gather(tokens, gain, w_qkv, w_out):
    any_ = pl.BlockSpec(memory_space=pltpu.HBM)
    vm = pl.BlockSpec(memory_space=pltpu.VMEM)
    dma = pltpu.SemaphoreType.DMA
    return pl.pallas_call(
        gather_kernel,
        name="gather",
        out_shape=(
            pltpu.VMEM((N, D), BF16),
            pltpu.VMEM((3 * N, D), BF16),
            pltpu.VMEM((3 * N, D), BF16),
            pltpu.VMEM((HALF, 4 * D), BF16),
        ),
        in_specs=[any_, vm, any_, any_],
        out_specs=(vm,) * 4,
        scratch_shapes=[
            pltpu.VMEM((N, D), BF16),
            pltpu.VMEM((HALF, 4 * D), BF16),
            pltpu.VMEM((N, D), BF16),
            pltpu.VMEM((N, D), BF16),
            pltpu.VMEM((256, D), BF16),
            pltpu.VMEM((256, D), BF16),
            pltpu.VMEM((N, D), BF16),
            pltpu.VMEM((768, D), BF16),
            pltpu.VMEM((N, 3 * D), F32),
            pltpu.VMEM((768, 2 * D), F32),
            dma((72,)),
            dma((72,)),
            dma((24,)),
            dma((24,)),
            dma((3,)),
        ],
        compiler_params=pltpu.CompilerParams(
            collective_id=0, has_side_effects=True, vmem_limit_bytes=44 * MIB
        ),
    )(outside(tokens), gain, outside(w_qkv), outside(w_out))


def attend_kernel(
    lens_ref, q, k, v, wb, tok_hbm, wa_hbm,
    hid_hbm, part_ref,
    tok, wa, ctx, bias, hid, qid, kid, sems,
):
    sx, sy, d = lax.axis_index("sx"), lax.axis_index("sy"), lax.axis_index("dp")
    copies = [
        pltpu.make_async_copy(a, b, sems.at[i])
        for i, (a, b) in enumerate(
            ((tok_hbm, tok), (wa_hbm, wa))
        )
    ]
    for copy in copies:
        copy.start()
    first = (sx * 8 + sy) * N
    base = first - N

    lens = lens_ref[...].astype(F32)
    down = lax.broadcasted_iota(jnp.int32, (IMAGES, IMAGES), 0)
    along = lax.broadcasted_iota(jnp.int32, (IMAGES, IMAGES), 1)
    wide = jnp.broadcast_to(lens, (IMAGES, IMAGES))
    off_col = jnp.sum(jnp.where(along < down, wide, 0.0), axis=1, keepdims=True)
    len_col = jnp.sum(jnp.where(along == down, wide, 0.0), axis=1, keepdims=True)
    off_row = jnp.sum(
        jnp.where(down < along, jnp.broadcast_to(len_col, (IMAGES, IMAGES)), 0.0), axis=0, keepdims=True
    )
    for j in range(3):
        pos = (lax.broadcasted_iota(jnp.int32, (1, N), 1) + (base + j * N)).astype(F32)
        count = jnp.sum(jnp.where(off_col <= pos, 1.0, 0.0), axis=0, keepdims=True) - 1.0
        kid[:, pl.ds(j * N, N)] = jnp.where(pos < TOTAL, count, -1.0)
    for j in range(4):
        pos = (lax.broadcasted_iota(jnp.int32, (128, 1), 0) + (first + j * 128)).astype(F32)
        qid[pl.ds(j * 128, 128), :] = jnp.sum(jnp.where(off_row <= pos, 1.0, 0.0), axis=1, keepdims=True) - 1.0

    def block(i, _):
        rows = pl.ds(pl.multiple_of(i * 128, 128), 128)
        begin = (first + i * 128).astype(F32)
        low = jnp.max(jnp.where(off_row <= begin, off_row, 0.0)).astype(jnp.int32)
        high = jnp.min(jnp.where(off_row > begin + 127.0, off_row, float(TOTAL))).astype(jnp.int32)
        low = (low - base) >> 7
        high = (high - base + 127) >> 7
        blocks = high - low
        ids = qid[rows, :]
        before = 0
        for size in CLASSES:
            n = size * 128

            @pl.when((blocks > before) & (blocks <= size))
            def _():
                start = pl.multiple_of(jnp.minimum(low, 12 - size) * 128, 128)
                keys = pl.ds(start, n)
                bias[:, pl.ds(0, n)] = jnp.where(ids == kid[:, keys], 0.0, -1e30)

                several = 4 if size < 6 else 2

                def pairs(group, _):
                    work = []
                    for sub in range(several):
                        pair = group * several + sub
                        tile = (pair * 5) >> 2
                        lanes = pl.ds(pl.multiple_of(tile * 128, 128), 256)
                        shift = pair * 160 - tile * 128
                        lane = lax.broadcasted_iota(jnp.int32, (1, 256), 1) - shift
                        one = (lane >= 0) & (lane < SIZE)
                        two = (lane >= SIZE) & (lane < 2 * SIZE)
                        window = q[rows, lanes]
                        both = jnp.concatenate(
                            [
                                window * jnp.where(one, 1.0, 0.0).astype(BF16),
                                window * jnp.where(two, 1.0, 0.0).astype(BF16),
                            ],
                            axis=0,
                        )
                        scores = lax.dot_general(
                            both, k[keys, lanes], (((1,), (1,)), ((), ())), preferred_element_type=F32
                        )
                        work.append((lanes, one, two, scores))
                    done = []
                    for lanes, one, two, scores in work:
                        extra = bias[:, pl.ds(0, n)]
                        scores = scores + jnp.concatenate([extra, extra], axis=0)
                        top = jnp.max(scores, axis=1, keepdims=True)
                        weights = jnp.exp2(scores - top)
                        total = jnp.sum(weights, axis=1, keepdims=True)
                        mixed = jnp.dot(weights.astype(BF16), v[keys, lanes], preferred_element_type=F32)
                        done.append((lanes, one, two, mixed * (1.0 / total)))
                    for lanes, one, two, mixed in done:
                        old = ctx[rows, lanes].astype(F32)
                        ctx[rows, lanes] = jnp.where(one, mixed[:128], jnp.where(two, mixed[128:], old)).astype(BF16)
                    return 0

                lax.fori_loop(0, 8 // several, pairs, 0)

            before = size
        return 0

    lax.fori_loop(0, 4, block, 0)
    for copy in copies:
        copy.wait()
    mine = pl.ds(pl.multiple_of(d * HALF, 128), HALF)
    others = pl.ds(pl.multiple_of((1 - d) * HALF, 128), HALF)

    def project(i, _):
        rows = pl.ds(pl.multiple_of(i * 256, 256), 256)
        mixed = jnp.dot(ctx[rows, mine], wa[...], preferred_element_type=F32)
        mixed = mixed + jnp.dot(ctx[rows, others], wb[:, pl.ds(3 * D, D)], preferred_element_type=F32)
        hid[rows, :] = (tok[rows, :].astype(F32) + mixed).astype(BF16)
        return 0

    lax.fori_loop(0, 2, project, 0)
    out = pltpu.make_async_copy(hid, hid_hbm, sems.at[2])
    out.start()
    image = lax.broadcasted_iota(jnp.int32, (IMAGES, 1), 0).astype(F32)
    onehot = jnp.where(image == kid[:, pl.ds(N, N)], 1.0, 0.0).astype(BF16)
    sums = jnp.dot(onehot, hid[...], preferred_element_type=F32)
    part_ref[...] = (sums / len_col).astype(BF16)
    out.wait()


def attend(lengths, q, k, v, w_other, tokens, w_own):
    any_ = pl.BlockSpec(memory_space=pltpu.HBM)
    vm = pl.BlockSpec(memory_space=pltpu.VMEM)
    return pl.pallas_call(
        attend_kernel,
        name="attend",
        out_shape=(
            jax.ShapeDtypeStruct((N, D), BF16),
            pltpu.VMEM((IMAGES, D), BF16),
        ),
        in_specs=[vm] * 5 + [any_] * 2,
        out_specs=(any_, vm),
        scratch_shapes=[
            pltpu.VMEM((N, D), BF16),
            pltpu.VMEM((HALF, D), BF16),
            pltpu.VMEM((N, D), BF16),
            pltpu.VMEM((128, 128 * CLASSES[-1]), F32),
            pltpu.VMEM((N, D), BF16),
            pltpu.VMEM((N, 1), F32),
            pltpu.VMEM((1, 3 * N), F32),
            pltpu.SemaphoreType.DMA((3,)),
        ],
        compiler_params=pltpu.CompilerParams(vmem_limit_bytes=28 * MIB),
    )(lengths, *[held(x) for x in (q, k, v, w_other)], outside(tokens), outside(w_own))


def combine_kernel(
    part, out, rc, one, rx, two, ry, three, four, last,
    c_send, c_recv, x_send, x_recv, y_send, y_recv, g_send, g_recv, w_send, w_recv,
):
    sx, sy, d = lax.axis_index("sx"), lax.axis_index("sy"), lax.axis_index("dp")
    core = lax.rem(sx, 2)
    chip = sx // 2
    mate = (sx + 1 - 2 * core, sy, d)
    chips = [(lax.rem(sx + 2 * j, 8), sy, d) for j in (1, 2, 3)]
    plane = [(sx, lax.rem(sy + j, 8), d) for j in range(1, 8)]
    barrier = pltpu.get_barrier_semaphore()
    for who in [mate] + chips + plane:
        pl.semaphore_signal(barrier, inc=1, device_id=who, device_id_type=MESH)
    pl.semaphore_wait(barrier, 11)

    def remote(src, dst, send, recv, who):
        return pltpu.make_async_remote_copy(
            src_ref=src, dst_ref=dst, send_sem=send, recv_sem=recv, device_id=who, device_id_type=MESH
        )

    my_half = pl.ds(pl.multiple_of(core * 128, 128), 128)
    its_half = pl.ds(pl.multiple_of((1 - core) * 128, 128), 128)
    c_copy = remote(part.at[its_half], rc, c_send.at[0], c_recv.at[0], mate)
    c_copy.start()
    c_copy.wait_recv()
    one[...] = (part[my_half, :].astype(F32) + rc[...].astype(F32)).astype(BF16)

    def strip(owner):
        return pl.ds(pl.multiple_of(owner * 32, 32), 32)

    x_copies = [
        remote(one.at[strip(lax.rem(chip + j, 4))], rx.at[j - 1], x_send.at[j - 1], x_recv.at[j - 1], chips[j - 1])
        for j in (1, 2, 3)
    ]
    for copy in x_copies:
        copy.start()
    for copy in x_copies:
        copy.wait_recv()
    total = one[strip(chip), :].astype(F32)
    for j in range(3):
        total = total + rx[j].astype(F32)
    for j in range(2):
        two[j] = total[:, j * HALF : (j + 1) * HALF]

    def spot(owner):
        return pl.ds(pl.multiple_of((owner // 2) * 8, 8), 8)

    y_copies = []
    for j in range(1, 8):
        to = lax.rem(sy + j, 8)
        y_copies.append(
            remote(two.at[lax.rem(to, 2), spot(to)], ry.at[j - 1], y_send.at[j - 1], y_recv.at[j - 1], plane[j - 1])
        )
    for copy in y_copies:
        copy.start()
    for copy in y_copies:
        copy.wait_recv()
    side = lax.rem(sy, 2)
    total = two[side, spot(sy), :]
    for j in range(7):
        total = total + ry[j]
    three[side, spot(sy), :] = total
    g_copies = [
        remote(three.at[side, spot(sy)], three.at[side, spot(sy)], g_send.at[j], g_recv.at[j], plane[j])
        for j in range(7)
    ]
    for copy in g_copies:
        copy.start()
    for copy in g_copies:
        copy.wait_recv()
    four[strip(chip), :] = jnp.concatenate([three[0], three[1]], axis=1).astype(BF16)
    w_copies = [
        remote(four.at[strip(chip)], four.at[strip(chip)], w_send.at[j], w_recv.at[j], chips[j]) for j in range(3)
    ]
    for copy in w_copies:
        copy.start()
    for copy in w_copies:
        copy.wait_recv()
    l_copy = remote(four, last, c_send.at[1], c_recv.at[1], mate)
    l_copy.start()
    out[my_half, :] = four[...].astype(F32)
    l_copy.wait_recv()
    out[its_half, :] = last[...].astype(F32)
    for copy in [c_copy, l_copy] + x_copies + y_copies + g_copies + w_copies:
        copy.wait_send()


def combine(part):
    vm = pl.BlockSpec(memory_space=pltpu.VMEM)
    dma = pltpu.SemaphoreType.DMA
    return pl.pallas_call(
        combine_kernel,
        name="combine",
        out_shape=pltpu.VMEM((IMAGES, D), F32),
        in_specs=[vm],
        out_specs=vm,
        scratch_shapes=[
            pltpu.VMEM((128, D), BF16),
            pltpu.VMEM((128, D), BF16),
            pltpu.VMEM((3, 32, D), BF16),
            pltpu.VMEM((2, 32, HALF), F32),
            pltpu.VMEM((7, 8, HALF), F32),
            pltpu.VMEM((2, 32, HALF), F32),
            pltpu.VMEM((128, D), BF16),
            pltpu.VMEM((128, D), BF16),
            dma((2,)),
            dma((2,)),
            dma((3,)),
            dma((3,)),
            dma((7,)),
            dma((7,)),
            dma((7,)),
            dma((7,)),
            dma((3,)),
            dma((3,)),
        ],
        compiler_params=pltpu.CompilerParams(
            collective_id=1, has_side_effects=True, vmem_limit_bytes=8 * MIB
        ),
    )(held(part))


def shards(tokens, lengths, ln_gain, w_qkv, w_out):
    rows = tokens.reshape(N, D)
    q, k, v, w_other = gather(rows, ln_gain, w_qkv, w_out)
    hidden, part = attend(lengths, q, k, v, w_other, rows, w_out)
    pooled = combine(part)
    return hidden.reshape(1, N, D), pooled.reshape(1, IMAGES, D)


def solution(mesh):
    in_specs = (P("dp", ("sx", "sy"), None), P("dp", None), P(), P("dp", None), P("dp", None))
    out_specs = (P("dp", ("sx", "sy"), None), P("dp", None, None))
    return jax.shard_map(shards, mesh=mesh, in_specs=in_specs, out_specs=out_specs, check_vma=False)
```

```python
import math

import jax
import jax.numpy as jnp
from jax import lax
from jax.experimental import pallas as pl
from jax.experimental.pallas import tpu as pltpu
from jax.sharding import PartitionSpec as P

MESH = pl.DeviceIdType.MESH
F32 = jnp.float32
BF16 = jnp.bfloat16
D = 1280
HALF = 640
N = 512
SIZE = 80
IMAGES = 256
TOTAL = 32768
SCALE = SIZE**-0.5 * math.log2(math.e)
PIECE = 80
CLASSES = (2, 3, 4, 5, 6, 9)
MIB = 1024 * 1024


def places():
    sx, sy, d = lax.axis_index("sx"), lax.axis_index("sy"), lax.axis_index("dp")
    h = lax.rem(sy, 2)
    flip = sy + 1 - 2 * h
    shard = sx * 8 + sy
    onward = lax.rem(shard + 2 - 4 * h + 64, 64)
    back = lax.rem(shard - 2 + 4 * h + 64, 64)
    mate = sx + 1 - 2 * lax.rem(sx, 2)
    where = {
        "a": (sx, sy, 1 - d),
        "b": (sx, flip, 1 - d),
        "xp": (lax.rem(sx + 2, 8), sy, d),
        "xm": (lax.rem(sx + 6, 8), sy, d),
        "core": (mate, sy, d),
        "z": (onward // 8, lax.rem(onward, 8), d),
        "zb": (back // 8, lax.rem(back, 8), d),
        "zi": (sx, lax.rem(sy + 6 + 4 * h, 8), d),
        "zj": (sx, lax.rem(sy + 10 - 4 * h, 8), d),
    }
    z = sy // 2
    first, last = (3 - z) // 3, z // 3
    where["hop"] = (6 - 4 * h * first, 2 + 4 * (1 - h) * last)
    return sx, sy, d, h, mate, where


def normalize(rows, gain):
    values = rows.astype(F32)
    center = values - jnp.mean(values, axis=-1, keepdims=True)
    spread = jnp.mean(center * center, axis=-1, keepdims=True)
    return (center * lax.rsqrt(spread + 1e-05) * gain).astype(BF16)


class Exchange:
    def __init__(self, own, other, sx, z, turn, where, send, recv):
        self.own, self.other, self.sx, self.z, self.turn = own, other, sx, z, turn
        self.where, self.send, self.recv = where, send, recv

    def copy(self, kind, t, side):
        pair = lax.rem(self.z + self.turn * (t - (kind == 8)) + 8, 4)
        chunk = pair + 3 + pair // 3 if side else pair + 3 * (pair // 3)
        cols = pl.ds(pl.multiple_of(chunk * HALF, 128), HALF)
        own, other, where = self.own, self.other, self.where
        hop = where["hop"][side] if t else (6, 2)[side]
        ahead, src, to = (
            (0, own, where["b" if side else "a"]),
            (0, other, where["xp"]),
            (0, other, where["xm"]),
            (0, other, where["core"]),
            (8 - hop, other, (lax.rem(self.sx + hop, 8),) + where["core"][1:]),
            (2, other, where["core"]),
            (6, other, where["core"]),
            (4, other, where["core"]),
            (0, other, where["zi"]),
        )[kind]
        rows = pl.ds(pl.multiple_of(lax.rem(self.sx + ahead, 8) * PIECE, 16), PIECE)
        i = kind * 8 + side * 4 + t
        return pltpu.make_async_remote_copy(
            src_ref=src.at[rows, cols],
            dst_ref=other.at[rows, cols],
            send_sem=self.send.at[i],
            recv_sem=self.recv.at[i],
            device_id=to,
            device_id_type=MESH,
        )

    def begin(self):
        for side in range(2):
            self.copy(0, 0, side).start()

    def landed(self, t):
        for side in range(2):
            self.copy(8 if t else 0, t, side).wait_recv()
            if t < 3:
                self.copy(8, t + 1, side).start()
            for kind in (1, 2, 3):
                self.copy(kind, t, side).start()

    def from_x(self, t):
        for side in range(2):
            for kind in (1, 2):
                self.copy(kind, t, side).wait_recv()
            for kind in (4, 5, 6):
                self.copy(kind, t, side).start()

    def from_far(self, t):
        for side in range(2):
            self.copy(4, t, side).wait_recv()
            self.copy(7, t, side).start()

    def finish(self):
        for t in range(4):
            for side in range(2):
                for kind in (3, 5, 6, 7):
                    self.copy(kind, t, side).wait_recv()

    def sent(self):
        for side in range(2):
            for t in range(4):
                for kind in range(1, 8):
                    self.copy(kind, t, side).wait_send()
                self.copy(8 if t else 0, t, side).wait_send()


class Halo:
    def __init__(self, tok, ta, tb, near, far, where, send, recv):
        self.table = []
        for i in range(4):
            self.table += [(tok, i, ta, i, "a"), (tok, 4 + i, tb, i, "b")]
        for i in range(4):
            self.table += [(ta, i, near, i, "b"), (tb, i, near, 4 + i, "a")]
        for i in range(4):
            self.table += [(near, i, far, i, "z"), (near, 4 + i, far, 4 + i, "z")]
        self.where, self.send, self.recv = where, send, recv

    def copy(self, i):
        src, at, dst, to, name = self.table[i]
        return pltpu.make_async_remote_copy(
            src_ref=src.at[pl.ds(64 * at, 64)],
            dst_ref=dst.at[pl.ds(64 * to, 64)],
            send_sem=self.send.at[i],
            recv_sem=self.recv.at[i],
            device_id=self.where[name],
            device_id_type=MESH,
        )

    def own(self, i):
        self.copy(2 * i).start()
        self.copy(2 * i + 1).start()

    def relay(self, i):
        for j in (2 * i, 2 * i + 1):
            self.copy(j).wait_recv()
            self.copy(8 + j).start()

    def onward(self, i):
        for j in (2 * i, 2 * i + 1):
            self.copy(8 + j).wait_recv()
            self.copy(16 + j).start()

    def arrived(self, i):
        for j in (2 * i, 2 * i + 1):
            self.copy(16 + j).wait_recv()

    def sent(self):
        for i in range(24):
            self.copy(i).wait_send()


def gather_kernel(
    tok_hbm, gain_ref, wq_hbm, wo_hbm,
    qs, ks, vs, wall,
    tok, wown, near, far, ta, tb, nrm, nrmh, acc, acch,
    w_send, w_recv, h_send, h_recv, local,
):
    sx, sy, d, h, mate, where = places()
    wq_in = pltpu.make_async_copy(wq_hbm, wown.at[:, pl.ds(0, 3 * D)], local.at[1])
    wo_in = pltpu.make_async_copy(wo_hbm, wown.at[:, pl.ds(3 * D, D)], local.at[2])
    tok_in = pltpu.make_async_copy(tok_hbm, tok, local.at[0])
    wq_in.start()
    wo_in.start()
    tok_in.start()
    barrier = pltpu.get_barrier_semaphore()
    partners = ("a", "b", "xp", "xm", "core", "z", "zb", "zi", "zj")
    for name in partners:
        pl.semaphore_signal(barrier, inc=1, device_id=where[name], device_id_type=MESH)
    wq_in.wait()
    wo_in.wait()
    pl.semaphore_wait(barrier, len(partners))

    weights = Exchange(wown, wall, sx, sy // 2, 1 - 2 * h, where, w_send, w_recv)
    halo = Halo(tok_hbm, ta, tb, near, far, where, h_send, h_recv)
    gain = gain_ref[...].reshape(1, D)
    mine = pl.ds(pl.multiple_of(d * HALF, 128), HALF)
    others = pl.ds(pl.multiple_of((1 - d) * HALF, 128), HALF)
    near_at = (1 - h) * (2 * N)
    far_at = h * (2 * N)

    def norm_own(i, _):
        rows = pl.ds(pl.multiple_of(i * 64, 64), 64)
        nrm[rows, :] = normalize(tok[rows, :], gain)
        return 0

    def first_half(part):
        def one(i, _):
            rows = pl.ds(pl.multiple_of(i * 256, 256), 256)
            cols = pl.ds(part * D, D)
            acc[rows, cols] = jnp.dot(nrm[rows, mine], wown[:, cols], preferred_element_type=F32)
            return 0

        lax.fori_loop(0, 2, one, 0)

    def second_half(i, _):
        rows = pl.ds(pl.multiple_of(i * 256, 256), 256)
        into = pl.ds(pl.multiple_of(N + i * 256, 256), 256)
        for part, ref, at, factor in ((0, qs, rows, SCALE), (1, ks, into, None), (2, vs, into, None)):
            cols = pl.ds(part * D, D)
            value = acc[rows, cols] + jnp.dot(nrm[rows, others], wall[:, cols], preferred_element_type=F32)
            if factor is not None:
                value = value * factor
            ref[at, :] = value.astype(BF16)
        return 0

    def halo_first(src, first, group):
        def one(j, _):
            at = pl.multiple_of(128 * first + 64 * lax.rem(j, 2) + 256 * (j // 2), 64)
            to = pl.multiple_of(256 * group + 64 * j, 64)
            nrmh[pl.ds(to, 64), :] = normalize(src[pl.ds(at, 64), :], gain)
            return 0

        lax.fori_loop(0, 4, one, 0)
        rows = pl.ds(256 * group, 256)
        for part in range(2):
            acch[rows, pl.ds(part * D, D)] = jnp.dot(
                nrmh[rows, mine], wown[:, pl.ds((part + 1) * D, D)], preferred_element_type=F32
            )

    def halo_second(first, base, group):
        rows = pl.ds(256 * group, 256)
        for part, ref in ((0, ks), (1, vs)):
            value = acch[rows, pl.ds(part * D, D)] + jnp.dot(
                nrmh[rows, others], wall[:, pl.ds((part + 1) * D, D)], preferred_element_type=F32
            )
            for j in range(2):
                start = pl.multiple_of(base + 128 * first + 256 * j, 128)
                ref[pl.ds(start, 128), :] = value[128 * j : 128 * j + 128].astype(BF16)

    with jax.named_scope("g0"):
        weights.begin()
        halo.own(0)
        halo.own(1)
        tok_in.wait()
        lax.fori_loop(0, N // 64, norm_own, 0)
        weights.landed(0)
        first_half(0)
    with jax.named_scope("g1"):
        halo.relay(0)
        halo.own(2)
        first_half(1)
        weights.landed(1)
    with jax.named_scope("g2"):
        halo.relay(1)
        halo.own(3)
        first_half(2)
        weights.landed(2)
    with jax.named_scope("g3"):
        halo.onward(0)
        weights.from_x(0)
        weights.landed(3)
    with jax.named_scope("g4"):
        halo.relay(2)
        weights.from_x(1)
        halo.onward(1)
        weights.from_x(2)
    with jax.named_scope("g5"):
        halo_first(near, 0, 0)
        halo.relay(3)
    with jax.named_scope("g6"):
        weights.from_far(0)
        weights.from_x(3)
        halo.onward(2)
        weights.from_far(1)
        halo.onward(3)
    with jax.named_scope("g7"):
        weights.from_far(2)
        halo_first(near, 1, 1)
    with jax.named_scope("g8"):
        weights.from_far(3)
        halo.arrived(0)
        halo.arrived(1)
        halo_first(far, 0, 2)
        weights.finish()
    with jax.named_scope("g9"):
        lax.fori_loop(0, 2, second_half, 0)
        halo_second(0, near_at, 0)
        halo_second(1, near_at, 1)
        halo_second(0, far_at, 2)
    with jax.named_scope("g12"):
        halo.arrived(2)
        halo.arrived(3)
    with jax.named_scope("g13"):
        halo_first(far, 1, 0)
        halo_second(1, far_at, 0)
        weights.sent()
        halo.sent()


def held(x):
    return pltpu.with_memory_space_constraint(x, pltpu.VMEM)


def outside(x):
    return pltpu.with_memory_space_constraint(x, pltpu.HBM)


def gather(tokens, gain, w_qkv, w_out):
    any_ = pl.BlockSpec(memory_space=pltpu.HBM)
    vm = pl.BlockSpec(memory_space=pltpu.VMEM)
    dma = pltpu.SemaphoreType.DMA
    return pl.pallas_call(
        gather_kernel,
        name="gather",
        out_shape=(
            pltpu.VMEM((N, D), BF16),
            pltpu.VMEM((3 * N, D), BF16),
            pltpu.VMEM((3 * N, D), BF16),
            pltpu.VMEM((HALF, 4 * D), BF16),
        ),
        in_specs=[any_, vm, any_, any_],
        out_specs=(vm,) * 4,
        scratch_shapes=[
            pltpu.VMEM((N, D), BF16),
            pltpu.VMEM((HALF, 4 * D), BF16),
            pltpu.VMEM((N, D), BF16),
            pltpu.VMEM((N, D), BF16),
            pltpu.VMEM((256, D), BF16),
            pltpu.VMEM((256, D), BF16),
            pltpu.VMEM((N, D), BF16),
            pltpu.VMEM((768, D), BF16),
            pltpu.VMEM((N, 3 * D), F32),
            pltpu.VMEM((768, 2 * D), F32),
            dma((72,)),
            dma((72,)),
            dma((24,)),
            dma((24,)),
            dma((3,)),
        ],
        compiler_params=pltpu.CompilerParams(
            collective_id=0, has_side_effects=True, vmem_limit_bytes=44 * MIB
        ),
    )(outside(tokens), gain, outside(w_qkv), outside(w_out))


def attend_kernel(
    lens_ref, q, k, v, wb, tok_hbm, wa_hbm,
    hid_hbm, part_ref,
    tok, wa, ctx, bias, hid, qid, kid, sems,
):
    sx, sy, d = lax.axis_index("sx"), lax.axis_index("sy"), lax.axis_index("dp")
    copies = [
        pltpu.make_async_copy(a, b, sems.at[i])
        for i, (a, b) in enumerate(
            ((tok_hbm, tok), (wa_hbm, wa))
        )
    ]
    for copy in copies:
        copy.start()
    first = (sx * 8 + sy) * N
    base = first - N

    lens = lens_ref[...].astype(F32)
    down = lax.broadcasted_iota(jnp.int32, (IMAGES, IMAGES), 0)
    along = lax.broadcasted_iota(jnp.int32, (IMAGES, IMAGES), 1)
    wide = jnp.broadcast_to(lens, (IMAGES, IMAGES))
    off_col = jnp.sum(jnp.where(along < down, wide, 0.0), axis=1, keepdims=True)
    len_col = jnp.sum(jnp.where(along == down, wide, 0.0), axis=1, keepdims=True)
    off_row = jnp.sum(
        jnp.where(down < along, jnp.broadcast_to(len_col, (IMAGES, IMAGES)), 0.0), axis=0, keepdims=True
    )
    for j in range(3):
        pos = (lax.broadcasted_iota(jnp.int32, (1, N), 1) + (base + j * N)).astype(F32)
        count = jnp.sum(jnp.where(off_col <= pos, 1.0, 0.0), axis=0, keepdims=True) - 1.0
        kid[:, pl.ds(j * N, N)] = jnp.where(pos < TOTAL, count, -1.0)
    for j in range(4):
        pos = (lax.broadcasted_iota(jnp.int32, (128, 1), 0) + (first + j * 128)).astype(F32)
        qid[pl.ds(j * 128, 128), :] = jnp.sum(jnp.where(off_row <= pos, 1.0, 0.0), axis=1, keepdims=True) - 1.0

    def block(i, _):
        rows = pl.ds(pl.multiple_of(i * 128, 128), 128)
        begin = (first + i * 128).astype(F32)
        low = jnp.max(jnp.where(off_row <= begin, off_row, 0.0)).astype(jnp.int32)
        high = jnp.min(jnp.where(off_row > begin + 127.0, off_row, float(TOTAL))).astype(jnp.int32)
        low = (low - base) >> 7
        high = (high - base + 127) >> 7
        blocks = high - low
        ids = qid[rows, :]
        before = 0
        for size in CLASSES:
            n = size * 128

            @pl.when((blocks > before) & (blocks <= size))
            def _():
                start = pl.multiple_of(jnp.minimum(low, 12 - size) * 128, 128)
                keys = pl.ds(start, n)
                bias[:, pl.ds(0, n)] = jnp.where(ids == kid[:, keys], 0.0, -1e30)

                several = 4 if size < 6 else 2

                def pairs(group, _):
                    work = []
                    for sub in range(several):
                        pair = group * several + sub
                        tile = (pair * 5) >> 2
                        lanes = pl.ds(pl.multiple_of(tile * 128, 128), 256)
                        shift = pair * 160 - tile * 128
                        lane = lax.broadcasted_iota(jnp.int32, (1, 256), 1) - shift
                        one = (lane >= 0) & (lane < SIZE)
                        two = (lane >= SIZE) & (lane < 2 * SIZE)
                        window = q[rows, lanes]
                        both = jnp.concatenate(
                            [
                                window * jnp.where(one, 1.0, 0.0).astype(BF16),
                                window * jnp.where(two, 1.0, 0.0).astype(BF16),
                            ],
                            axis=0,
                        )
                        scores = lax.dot_general(
                            both, k[keys, lanes], (((1,), (1,)), ((), ())), preferred_element_type=F32
                        )
                        extra = bias[:, pl.ds(0, n)]
                        scores = scores + jnp.concatenate([extra, extra], axis=0)
                        work.append((lanes, one, two, scores, jnp.max(scores, axis=1, keepdims=True)))
                    done = []
                    for lanes, one, two, scores, top in work:
                        weights = jnp.exp2(scores - top)
                        total = jnp.sum(weights, axis=1, keepdims=True)
                        mixed = jnp.dot(weights.astype(BF16), v[keys, lanes], preferred_element_type=F32)
                        done.append((lanes, one, two, mixed * (1.0 / total)))
                    for lanes, one, two, mixed in done:
                        old = ctx[rows, lanes].astype(F32)
                        ctx[rows, lanes] = jnp.where(one, mixed[:128], jnp.where(two, mixed[128:], old)).astype(BF16)
                    return 0

                lax.fori_loop(0, 8 // several, pairs, 0)

            before = size
        return 0

    lax.fori_loop(0, 4, block, 0)
    for copy in copies:
        copy.wait()
    mine = pl.ds(pl.multiple_of(d * HALF, 128), HALF)
    others = pl.ds(pl.multiple_of((1 - d) * HALF, 128), HALF)

    def project(i, _):
        rows = pl.ds(pl.multiple_of(i * 256, 256), 256)
        mixed = jnp.dot(ctx[rows, mine], wa[...], preferred_element_type=F32)
        mixed = mixed + jnp.dot(ctx[rows, others], wb[:, pl.ds(3 * D, D)], preferred_element_type=F32)
        hid[rows, :] = (tok[rows, :].astype(F32) + mixed).astype(BF16)
        return 0

    lax.fori_loop(0, 2, project, 0)
    out = pltpu.make_async_copy(hid, hid_hbm, sems.at[2])
    out.start()
    image = lax.broadcasted_iota(jnp.int32, (IMAGES, 1), 0).astype(F32)
    onehot = jnp.where(image == kid[:, pl.ds(N, N)], 1.0, 0.0).astype(BF16)
    sums = jnp.dot(onehot, hid[...], preferred_element_type=F32)
    part_ref[...] = (sums / len_col).astype(BF16)
    out.wait()


def attend(lengths, q, k, v, w_other, tokens, w_own):
    any_ = pl.BlockSpec(memory_space=pltpu.HBM)
    vm = pl.BlockSpec(memory_space=pltpu.VMEM)
    return pl.pallas_call(
        attend_kernel,
        name="attend",
        out_shape=(
            jax.ShapeDtypeStruct((N, D), BF16),
            pltpu.VMEM((IMAGES, D), BF16),
        ),
        in_specs=[vm] * 5 + [any_] * 2,
        out_specs=(any_, vm),
        scratch_shapes=[
            pltpu.VMEM((N, D), BF16),
            pltpu.VMEM((HALF, D), BF16),
            pltpu.VMEM((N, D), BF16),
            pltpu.VMEM((128, 128 * CLASSES[-1]), F32),
            pltpu.VMEM((N, D), BF16),
            pltpu.VMEM((N, 1), F32),
            pltpu.VMEM((1, 3 * N), F32),
            pltpu.SemaphoreType.DMA((3,)),
        ],
        compiler_params=pltpu.CompilerParams(vmem_limit_bytes=28 * MIB),
    )(lengths, *[held(x) for x in (q, k, v, w_other)], outside(tokens), outside(w_own))


def combine_kernel(part, out, rc, one, rx, two, ry, three, strip32, four, last, send, recv):
    sx, sy, d = lax.axis_index("sx"), lax.axis_index("sy"), lax.axis_index("dp")
    core = lax.rem(sx, 2)
    chip = sx // 2
    mate = (sx + 1 - 2 * core, sy, d)
    chips = [(lax.rem(sx + 2 * j, 8), sy, d) for j in (1, 2, 3)]
    plane = [(sx, lax.rem(sy + j, 8), d) for j in range(1, 8)]
    barrier = pltpu.get_barrier_semaphore()
    for who in [mate] + chips + plane:
        pl.semaphore_signal(barrier, inc=1, device_id=who, device_id_type=MESH)
    pl.semaphore_wait(barrier, 11)

    my_half = pl.ds(pl.multiple_of(core * 128, 128), 128)
    its_half = pl.ds(pl.multiple_of((1 - core) * 128, 128), 128)
    halves = [pl.ds(half * HALF, HALF) for half in range(2)]

    def strip(ahead):
        return pl.ds(pl.multiple_of(lax.rem(chip + ahead, 4) * 32, 32), 32)

    def remote(i, half, src, dst, who):
        return pltpu.make_async_remote_copy(
            src_ref=src,
            dst_ref=dst,
            send_sem=send.at[25 * half + i],
            recv_sem=recv.at[25 * half + i],
            device_id=who,
            device_id_type=MESH,
        )

    copies = {}
    for half in range(2):
        copies["c", half] = [remote(0, half, part.at[its_half, halves[half]], rc.at[half], mate)]
        copies["x", half] = [
            remote(j, half, one.at[half, strip(j)], rx.at[half, j - 1], chips[j - 1]) for j in (1, 2, 3)
        ]
        copies["p", half] = [
            remote(3 + j, half, two.at[half, lax.rem(sy + j, 8)], ry.at[half, j - 1], plane[j - 1])
            for j in range(1, 8)
        ]
        copies["g", half] = [
            remote(10 + j, half, three.at[half, sy], three.at[half, sy], plane[j - 1]) for j in range(1, 8)
        ]
        copies["w", half] = [
            remote(17 + j, half, four.at[half, strip(0)], four.at[half, strip(0)], chips[j - 1]) for j in (1, 2, 3)
        ]
        copies["m", half] = [
            remote(21 + j, half, four.at[half, strip(4 - j)], last.at[half, strip(4 - j)], mate) for j in range(4)
        ]

    def go(name, half):
        for copy in copies[name, half]:
            copy.start()

    def arrived(name, half):
        for copy in copies[name, half]:
            copy.wait_recv()

    for half in range(2):
        go("c", half)
    for half in range(2):
        arrived("c", half)
        one[half] = (part[my_half, halves[half]].astype(F32) + rc[half].astype(F32)).astype(BF16)
        go("x", half)
    for half in range(2):
        arrived("x", half)
        total = one[half, strip(0), :].astype(F32)
        for j in range(3):
            total = total + rx[half, j].astype(F32)
        for j in range(8):
            two[half, j] = total[4 * j : 4 * j + 4]
        go("p", half)
    for half in range(2):
        arrived("p", half)
        total = two[half, sy]
        for j in range(7):
            total = total + ry[half, j]
        three[half, sy] = total
        go("g", half)
    for half in range(2):
        arrived("g", half)
        for j in range(8):
            strip32[pl.ds(4 * j, 4), :] = three[half, j]
        four[half, strip(0), :] = strip32[...].astype(BF16)
        go("w", half)
        copies["m", half][0].start()
    for half in range(2):
        for j in (1, 3, 2):
            copies["w", half][j - 1].wait_recv()
            copies["m", half][j].start()
        out[my_half, halves[half]] = four[half].astype(F32)
    for half in range(2):
        arrived("m", half)
        out[its_half, halves[half]] = last[half].astype(F32)
    for group in copies.values():
        for copy in group:
            copy.wait_send()


def combine(part):
    vm = pl.BlockSpec(memory_space=pltpu.VMEM)
    dma = pltpu.SemaphoreType.DMA
    return pl.pallas_call(
        combine_kernel,
        name="combine",
        out_shape=pltpu.VMEM((IMAGES, D), F32),
        in_specs=[vm],
        out_specs=vm,
        scratch_shapes=[
            pltpu.VMEM((2, 128, HALF), BF16),
            pltpu.VMEM((2, 128, HALF), BF16),
            pltpu.VMEM((2, 3, 32, HALF), BF16),
            pltpu.VMEM((2, 8, 4, HALF), F32),
            pltpu.VMEM((2, 7, 4, HALF), F32),
            pltpu.VMEM((2, 8, 4, HALF), F32),
            pltpu.VMEM((32, HALF), F32),
            pltpu.VMEM((2, 128, HALF), BF16),
            pltpu.VMEM((2, 128, HALF), BF16),
            dma((50,)),
            dma((50,)),
        ],
        compiler_params=pltpu.CompilerParams(
            collective_id=1, has_side_effects=True, vmem_limit_bytes=8 * MIB
        ),
    )(held(part))


def shards(tokens, lengths, ln_gain, w_qkv, w_out):
    rows = tokens.reshape(N, D)
    q, k, v, w_other = gather(rows, ln_gain, w_qkv, w_out)
    hidden, part = attend(lengths, q, k, v, w_other, rows, w_out)
    pooled = combine(part)
    return hidden.reshape(1, N, D), pooled.reshape(1, IMAGES, D)


def solution(mesh):
    in_specs = (P("dp", ("sx", "sy"), None), P("dp", None), P(), P("dp", None), P("dp", None))
    out_specs = (P("dp", ("sx", "sy"), None), P("dp", None, None))
    return jax.shard_map(shards, mesh=mesh, in_specs=in_specs, out_specs=out_specs, check_vma=False)
```

```python
import math

import jax
import jax.numpy as jnp
from jax import lax
from jax.experimental import pallas as pl
from jax.experimental.pallas import tpu as pltpu
from jax.sharding import PartitionSpec as P

MESH = pl.DeviceIdType.MESH
F32 = jnp.float32
BF16 = jnp.bfloat16
D = 1280
HALF = 640
N = 512
SIZE = 80
IMAGES = 256
TOTAL = 32768
SCALE = SIZE**-0.5 * math.log2(math.e)
PIECE = 80
CLASSES = (2, 3, 4, 5, 6, 9)
MIB = 1024 * 1024


def places():
    sx, sy, d = lax.axis_index("sx"), lax.axis_index("sy"), lax.axis_index("dp")
    h = lax.rem(sy, 2)
    flip = sy + 1 - 2 * h
    shard = sx * 8 + sy
    onward = lax.rem(shard + 2 - 4 * h + 64, 64)
    back = lax.rem(shard - 2 + 4 * h + 64, 64)
    mate = sx + 1 - 2 * lax.rem(sx, 2)
    where = {
        "a": (sx, sy, 1 - d),
        "b": (sx, flip, 1 - d),
        "xp": (lax.rem(sx + 2, 8), sy, d),
        "xm": (lax.rem(sx + 6, 8), sy, d),
        "core": (mate, sy, d),
        "z": (onward // 8, lax.rem(onward, 8), d),
        "zb": (back // 8, lax.rem(back, 8), d),
        "zi": (sx, lax.rem(sy + 6 + 4 * h, 8), d),
        "zj": (sx, lax.rem(sy + 10 - 4 * h, 8), d),
    }
    z = sy // 2
    first, last = (3 - z) // 3, z // 3
    where["hop"] = (6 - 4 * h * first, 2 + 4 * (1 - h) * last)
    return sx, sy, d, h, mate, where


def normalize(rows, gain):
    values = rows.astype(F32)
    center = values - jnp.mean(values, axis=-1, keepdims=True)
    spread = jnp.mean(center * center, axis=-1, keepdims=True)
    return (center * lax.rsqrt(spread + 1e-05) * gain).astype(BF16)


class Exchange:
    def __init__(self, own, other, sx, z, turn, where, send, recv):
        self.own, self.other, self.sx, self.z, self.turn = own, other, sx, z, turn
        self.where, self.send, self.recv = where, send, recv

    def copy(self, kind, t, side):
        pair = lax.rem(self.z + self.turn * (t - (kind == 8)) + 8, 4)
        chunk = pair + 3 + pair // 3 if side else pair + 3 * (pair // 3)
        cols = pl.ds(pl.multiple_of(chunk * HALF, 128), HALF)
        own, other, where = self.own, self.other, self.where
        hop = where["hop"][side] if t else (6, 2)[side]
        ahead, src, to = (
            (0, own, where["b" if side else "a"]),
            (0, other, where["xp"]),
            (0, other, where["xm"]),
            (0, other, where["core"]),
            (8 - hop, other, (lax.rem(self.sx + hop, 8),) + where["core"][1:]),
            (2, other, where["core"]),
            (6, other, where["core"]),
            (4, other, where["core"]),
            (0, other, where["zi"]),
        )[kind]
        rows = pl.ds(pl.multiple_of(lax.rem(self.sx + ahead, 8) * PIECE, 16), PIECE)
        i = kind * 8 + side * 4 + t
        return pltpu.make_async_remote_copy(
            src_ref=src.at[rows, cols],
            dst_ref=other.at[rows, cols],
            send_sem=self.send.at[i],
            recv_sem=self.recv.at[i],
            device_id=to,
            device_id_type=MESH,
        )

    def begin(self):
        for side in range(2):
            self.copy(0, 0, side).start()

    def landed(self, t):
        for side in range(2):
            self.copy(8 if t else 0, t, side).wait_recv()
            if t < 3:
                self.copy(8, t + 1, side).start()
            for kind in (1, 2, 3):
                self.copy(kind, t, side).start()

    def from_x(self, t):
        for side in range(2):
            for kind in (1, 2):
                self.copy(kind, t, side).wait_recv()
            for kind in (4, 5, 6):
                self.copy(kind, t, side).start()

    def from_far(self, t):
        for side in range(2):
            self.copy(4, t, side).wait_recv()
            self.copy(7, t, side).start()

    def finish(self):
        for t in range(4):
            for side in range(2):
                for kind in (3, 5, 6, 7):
                    self.copy(kind, t, side).wait_recv()

    def sent(self):
        for side in range(2):
            for t in range(4):
                for kind in range(1, 8):
                    self.copy(kind, t, side).wait_send()
                self.copy(8 if t else 0, t, side).wait_send()


class Halo:
    def __init__(self, tok, ta, tb, near, far, where, send, recv):
        self.table = []
        for i in range(4):
            self.table += [(tok, i, ta, i, "a"), (tok, 4 + i, tb, i, "b")]
        for i in range(4):
            self.table += [(ta, i, near, i, "b"), (tb, i, near, 4 + i, "a")]
        for i in range(4):
            self.table += [(near, i, far, i, "z"), (near, 4 + i, far, 4 + i, "z")]
        self.where, self.send, self.recv = where, send, recv

    def copy(self, i):
        src, at, dst, to, name = self.table[i]
        return pltpu.make_async_remote_copy(
            src_ref=src.at[pl.ds(64 * at, 64)],
            dst_ref=dst.at[pl.ds(64 * to, 64)],
            send_sem=self.send.at[i],
            recv_sem=self.recv.at[i],
            device_id=self.where[name],
            device_id_type=MESH,
        )

    def own(self, i):
        self.copy(2 * i).start()
        self.copy(2 * i + 1).start()

    def relay(self, i):
        for j in (2 * i, 2 * i + 1):
            self.copy(j).wait_recv()
            self.copy(8 + j).start()

    def onward(self, i):
        for j in (2 * i, 2 * i + 1):
            self.copy(8 + j).wait_recv()
            self.copy(16 + j).start()

    def arrived(self, i):
        for j in (2 * i, 2 * i + 1):
            self.copy(16 + j).wait_recv()

    def sent(self):
        for i in range(24):
            self.copy(i).wait_send()


def gather_kernel(
    tok_hbm, gain_ref, wq_hbm, wo_hbm,
    qs, ks, vs, wall,
    tok, wown, near, far, ta, tb, nrm, nrmh, acc, acch,
    w_send, w_recv, h_send, h_recv, local,
):
    sx, sy, d, h, mate, where = places()
    wq_in = pltpu.make_async_copy(wq_hbm, wown.at[:, pl.ds(0, 3 * D)], local.at[1])
    wo_in = pltpu.make_async_copy(wo_hbm, wown.at[:, pl.ds(3 * D, D)], local.at[2])
    tok_in = pltpu.make_async_copy(tok_hbm, tok, local.at[0])
    wq_in.start()
    wo_in.start()
    tok_in.start()
    barrier = pltpu.get_barrier_semaphore()
    partners = ("a", "b", "xp", "xm", "core", "z", "zb", "zi", "zj")
    for name in partners:
        pl.semaphore_signal(barrier, inc=1, device_id=where[name], device_id_type=MESH)
    wq_in.wait()
    wo_in.wait()
    pl.semaphore_wait(barrier, len(partners))

    weights = Exchange(wown, wall, sx, sy // 2, 1 - 2 * h, where, w_send, w_recv)
    halo = Halo(tok_hbm, ta, tb, near, far, where, h_send, h_recv)
    gain = gain_ref[...].reshape(1, D)
    mine = pl.ds(pl.multiple_of(d * HALF, 128), HALF)
    others = pl.ds(pl.multiple_of((1 - d) * HALF, 128), HALF)
    near_at = (1 - h) * (2 * N)
    far_at = h * (2 * N)

    def norm_own(i, _):
        rows = pl.ds(pl.multiple_of(i * 64, 64), 64)
        nrm[rows, :] = normalize(tok[rows, :], gain)
        return 0

    def first_half(part):
        def one(i, _):
            rows = pl.ds(pl.multiple_of(i * 256, 256), 256)
            cols = pl.ds(part * D, D)
            acc[rows, cols] = jnp.dot(nrm[rows, mine], wown[:, cols], preferred_element_type=F32)
            return 0

        lax.fori_loop(0, 2, one, 0)

    def second_half(i, _):
        rows = pl.ds(pl.multiple_of(i * 256, 256), 256)
        into = pl.ds(pl.multiple_of(N + i * 256, 256), 256)
        for part, ref, at, factor in ((0, qs, rows, SCALE), (1, ks, into, None), (2, vs, into, None)):
            cols = pl.ds(part * D, D)
            value = acc[rows, cols] + jnp.dot(nrm[rows, others], wall[:, cols], preferred_element_type=F32)
            if factor is not None:
                value = value * factor
            ref[at, :] = value.astype(BF16)
        return 0

    def halo_first(src, first, group):
        def one(j, _):
            at = pl.multiple_of(128 * first + 64 * lax.rem(j, 2) + 256 * (j // 2), 64)
            to = pl.multiple_of(256 * group + 64 * j, 64)
            nrmh[pl.ds(to, 64), :] = normalize(src[pl.ds(at, 64), :], gain)
            return 0

        lax.fori_loop(0, 4, one, 0)
        rows = pl.ds(256 * group, 256)
        for part in range(2):
            acch[rows, pl.ds(part * D, D)] = jnp.dot(
                nrmh[rows, mine], wown[:, pl.ds((part + 1) * D, D)], preferred_element_type=F32
            )

    def halo_second(first, base, group):
        rows = pl.ds(256 * group, 256)
        for part, ref in ((0, ks), (1, vs)):
            value = acch[rows, pl.ds(part * D, D)] + jnp.dot(
                nrmh[rows, others], wall[:, pl.ds((part + 1) * D, D)], preferred_element_type=F32
            )
            for j in range(2):
                start = pl.multiple_of(base + 128 * first + 256 * j, 128)
                ref[pl.ds(start, 128), :] = value[128 * j : 128 * j + 128].astype(BF16)

    with jax.named_scope("g0"):
        weights.begin()
        halo.own(0)
        halo.own(1)
        tok_in.wait()
        lax.fori_loop(0, N // 64, norm_own, 0)
        weights.landed(0)
        first_half(0)
    with jax.named_scope("g1"):
        halo.relay(0)
        halo.own(2)
        first_half(1)
        weights.landed(1)
    with jax.named_scope("g2"):
        halo.relay(1)
        halo.own(3)
        first_half(2)
        weights.landed(2)
    with jax.named_scope("g3"):
        halo.onward(0)
        weights.from_x(0)
        weights.landed(3)
    with jax.named_scope("g4"):
        halo.relay(2)
        weights.from_x(1)
        halo.onward(1)
        weights.from_x(2)
    with jax.named_scope("g5"):
        halo_first(near, 0, 0)
        halo.relay(3)
    with jax.named_scope("g6"):
        weights.from_far(0)
        weights.from_x(3)
        halo.onward(2)
        weights.from_far(1)
        halo.onward(3)
    with jax.named_scope("g7"):
        weights.from_far(2)
        halo_first(near, 1, 1)
    with jax.named_scope("g8"):
        weights.from_far(3)
        halo.arrived(0)
        halo.arrived(1)
        halo_first(far, 0, 2)
        weights.finish()
    with jax.named_scope("g9"):
        lax.fori_loop(0, 2, second_half, 0)
        halo_second(0, near_at, 0)
        halo_second(1, near_at, 1)
        halo_second(0, far_at, 2)
    with jax.named_scope("g12"):
        halo.arrived(2)
        halo.arrived(3)
    with jax.named_scope("g13"):
        halo_first(far, 1, 0)
        halo_second(1, far_at, 0)
        weights.sent()
        halo.sent()


def held(x):
    return pltpu.with_memory_space_constraint(x, pltpu.VMEM)


def outside(x):
    return pltpu.with_memory_space_constraint(x, pltpu.HBM)


def gather(tokens, gain, w_qkv, w_out):
    any_ = pl.BlockSpec(memory_space=pltpu.HBM)
    vm = pl.BlockSpec(memory_space=pltpu.VMEM)
    dma = pltpu.SemaphoreType.DMA
    return pl.pallas_call(
        gather_kernel,
        name="gather",
        out_shape=(
            pltpu.VMEM((N, D), BF16),
            pltpu.VMEM((3 * N, D), BF16),
            pltpu.VMEM((3 * N, D), BF16),
            pltpu.VMEM((HALF, 4 * D), BF16),
        ),
        in_specs=[any_, vm, any_, any_],
        out_specs=(vm,) * 4,
        scratch_shapes=[
            pltpu.VMEM((N, D), BF16),
            pltpu.VMEM((HALF, 4 * D), BF16),
            pltpu.VMEM((N, D), BF16),
            pltpu.VMEM((N, D), BF16),
            pltpu.VMEM((256, D), BF16),
            pltpu.VMEM((256, D), BF16),
            pltpu.VMEM((N, D), BF16),
            pltpu.VMEM((768, D), BF16),
            pltpu.VMEM((N, 3 * D), F32),
            pltpu.VMEM((768, 2 * D), F32),
            dma((72,)),
            dma((72,)),
            dma((24,)),
            dma((24,)),
            dma((3,)),
        ],
        compiler_params=pltpu.CompilerParams(
            collective_id=0, has_side_effects=True, vmem_limit_bytes=44 * MIB
        ),
    )(outside(tokens), gain, outside(w_qkv), outside(w_out))


def attend_kernel(
    lens_ref, q, k, v, wb, tok_hbm, wa_hbm,
    hid_hbm, part_ref,
    tok, wa, ctx, bias, hid, qid, kid, sems,
):
    sx, sy, d = lax.axis_index("sx"), lax.axis_index("sy"), lax.axis_index("dp")
    copies = [
        pltpu.make_async_copy(a, b, sems.at[i])
        for i, (a, b) in enumerate(
            ((tok_hbm, tok), (wa_hbm, wa))
        )
    ]
    for copy in copies:
        copy.start()
    first = (sx * 8 + sy) * N
    base = first - N

    lens = lens_ref[...].astype(F32)
    down = lax.broadcasted_iota(jnp.int32, (IMAGES, IMAGES), 0)
    along = lax.broadcasted_iota(jnp.int32, (IMAGES, IMAGES), 1)
    wide = jnp.broadcast_to(lens, (IMAGES, IMAGES))
    off_col = jnp.sum(jnp.where(along < down, wide, 0.0), axis=1, keepdims=True)
    len_col = jnp.sum(jnp.where(along == down, wide, 0.0), axis=1, keepdims=True)
    off_row = jnp.sum(
        jnp.where(down < along, jnp.broadcast_to(len_col, (IMAGES, IMAGES)), 0.0), axis=0, keepdims=True
    )
    for j in range(3):
        pos = (lax.broadcasted_iota(jnp.int32, (1, N), 1) + (base + j * N)).astype(F32)
        count = jnp.sum(jnp.where(off_col <= pos, 1.0, 0.0), axis=0, keepdims=True) - 1.0
        kid[:, pl.ds(j * N, N)] = jnp.where(pos < TOTAL, count, -1.0)
    for j in range(4):
        pos = (lax.broadcasted_iota(jnp.int32, (128, 1), 0) + (first + j * 128)).astype(F32)
        qid[pl.ds(j * 128, 128), :] = jnp.sum(jnp.where(off_row <= pos, 1.0, 0.0), axis=1, keepdims=True) - 1.0

    def block(i, _):
        rows = pl.ds(pl.multiple_of(i * 128, 128), 128)
        begin = (first + i * 128).astype(F32)
        low = jnp.max(jnp.where(off_row <= begin, off_row, 0.0)).astype(jnp.int32)
        high = jnp.min(jnp.where(off_row > begin + 127.0, off_row, float(TOTAL))).astype(jnp.int32)
        low = (low - base) >> 7
        high = (high - base + 127) >> 7
        blocks = high - low
        ids = qid[rows, :]
        before = 0
        for size in CLASSES:
            n = size * 128

            @pl.when((blocks > before) & (blocks <= size))
            def _():
                start = pl.multiple_of(jnp.minimum(low, 12 - size) * 128, 128)
                keys = pl.ds(start, n)
                bias[:, pl.ds(0, n)] = jnp.where(ids == kid[:, keys], 0.0, -1e30)

                several = 8 if size < 6 else 4

                def pairs(group, _):
                    work, soft = {}, {}

                    def first(sub):
                        pair = group * several + sub
                        tile = (pair * 5) >> 2
                        lanes = pl.ds(pl.multiple_of(tile * 128, 128), 256)
                        shift = pair * 160 - tile * 128
                        lane = lax.broadcasted_iota(jnp.int32, (1, 256), 1) - shift
                        one = (lane >= 0) & (lane < SIZE)
                        two = (lane >= SIZE) & (lane < 2 * SIZE)
                        window = q[rows, lanes]
                        both = jnp.concatenate(
                            [
                                window * jnp.where(one, 1.0, 0.0).astype(BF16),
                                window * jnp.where(two, 1.0, 0.0).astype(BF16),
                            ],
                            axis=0,
                        )
                        scores = lax.dot_general(
                            both, k[keys, lanes], (((1,), (1,)), ((), ())), preferred_element_type=F32
                        )
                        extra = bias[:, pl.ds(0, n)]
                        scores = scores + jnp.concatenate([extra, extra], axis=0)
                        work[sub] = (lanes, one, two, scores, jnp.max(scores, axis=1, keepdims=True))

                    def middle(sub):
                        lanes, one, two, scores, top = work.pop(sub)
                        weights = jnp.exp2(scores - top)
                        total = jnp.sum(weights, axis=1, keepdims=True)
                        soft[sub] = (lanes, one, two, weights.astype(BF16), total)

                    def final(sub):
                        lanes, one, two, weights, total = soft.pop(sub)
                        mixed = jnp.dot(weights, v[keys, lanes], preferred_element_type=F32) * (1.0 / total)
                        old = ctx[rows, lanes].astype(F32)
                        ctx[rows, lanes] = jnp.where(one, mixed[:128], jnp.where(two, mixed[128:], old)).astype(BF16)

                    first(0)
                    for sub in range(several):
                        if sub + 1 < several:
                            first(sub + 1)
                        middle(sub)
                        if sub:
                            final(sub - 1)
                    final(several - 1)
                    return 0

                lax.fori_loop(0, 8 // several, pairs, 0)

            before = size
        return 0

    lax.fori_loop(0, 4, block, 0)
    for copy in copies:
        copy.wait()
    mine = pl.ds(pl.multiple_of(d * HALF, 128), HALF)
    others = pl.ds(pl.multiple_of((1 - d) * HALF, 128), HALF)

    def project(i, _):
        rows = pl.ds(pl.multiple_of(i * 256, 256), 256)
        mixed = jnp.dot(ctx[rows, mine], wa[...], preferred_element_type=F32)
        mixed = mixed + jnp.dot(ctx[rows, others], wb[:, pl.ds(3 * D, D)], preferred_element_type=F32)
        hid[rows, :] = (tok[rows, :].astype(F32) + mixed).astype(BF16)
        return 0

    lax.fori_loop(0, 2, project, 0)
    out = pltpu.make_async_copy(hid, hid_hbm, sems.at[2])
    out.start()
    image = lax.broadcasted_iota(jnp.int32, (IMAGES, 1), 0).astype(F32)
    onehot = jnp.where(image == kid[:, pl.ds(N, N)], 1.0, 0.0).astype(BF16)
    sums = jnp.dot(onehot, hid[...], preferred_element_type=F32)
    part_ref[...] = (sums / len_col).astype(BF16)
    out.wait()


def attend(lengths, q, k, v, w_other, tokens, w_own):
    any_ = pl.BlockSpec(memory_space=pltpu.HBM)
    vm = pl.BlockSpec(memory_space=pltpu.VMEM)
    return pl.pallas_call(
        attend_kernel,
        name="attend",
        out_shape=(
            jax.ShapeDtypeStruct((N, D), BF16),
            pltpu.VMEM((IMAGES, D), BF16),
        ),
        in_specs=[vm] * 5 + [any_] * 2,
        out_specs=(any_, vm),
        scratch_shapes=[
            pltpu.VMEM((N, D), BF16),
            pltpu.VMEM((HALF, D), BF16),
            pltpu.VMEM((N, D), BF16),
            pltpu.VMEM((128, 128 * CLASSES[-1]), F32),
            pltpu.VMEM((N, D), BF16),
            pltpu.VMEM((N, 1), F32),
            pltpu.VMEM((1, 3 * N), F32),
            pltpu.SemaphoreType.DMA((3,)),
        ],
        compiler_params=pltpu.CompilerParams(vmem_limit_bytes=28 * MIB),
    )(lengths, *[held(x) for x in (q, k, v, w_other)], outside(tokens), outside(w_own))


def combine_kernel(part, out, rc, one, rx, two, ry, three, strip32, four, last, send, recv):
    sx, sy, d = lax.axis_index("sx"), lax.axis_index("sy"), lax.axis_index("dp")
    core = lax.rem(sx, 2)
    chip = sx // 2
    mate = (sx + 1 - 2 * core, sy, d)
    chips = [(lax.rem(sx + 2 * j, 8), sy, d) for j in (1, 2, 3)]
    plane = [(sx, lax.rem(sy + j, 8), d) for j in range(1, 8)]
    barrier = pltpu.get_barrier_semaphore()
    for who in [mate] + chips + plane:
        pl.semaphore_signal(barrier, inc=1, device_id=who, device_id_type=MESH)
    pl.semaphore_wait(barrier, 11)

    my_half = pl.ds(pl.multiple_of(core * 128, 128), 128)
    its_half = pl.ds(pl.multiple_of((1 - core) * 128, 128), 128)
    halves = [pl.ds(half * HALF, HALF) for half in range(2)]

    def strip(ahead):
        return pl.ds(pl.multiple_of(lax.rem(chip + ahead, 4) * 32, 32), 32)

    def remote(i, half, src, dst, who):
        return pltpu.make_async_remote_copy(
            src_ref=src,
            dst_ref=dst,
            send_sem=send.at[25 * half + i],
            recv_sem=recv.at[25 * half + i],
            device_id=who,
            device_id_type=MESH,
        )

    copies = {}
    for half in range(2):
        copies["c", half] = [remote(0, half, part.at[its_half, halves[half]], rc.at[half], mate)]
        copies["x", half] = [
            remote(j, half, one.at[half, strip(j)], rx.at[half, j - 1], chips[j - 1]) for j in (1, 2, 3)
        ]
        copies["p", half] = [
            remote(3 + j, half, two.at[half, lax.rem(sy + j, 8)], ry.at[half, j - 1], plane[j - 1])
            for j in range(1, 8)
        ]
        copies["g", half] = [
            remote(10 + j, half, three.at[half, sy], three.at[half, sy], plane[j - 1]) for j in range(1, 8)
        ]
        copies["w", half] = [
            remote(17 + j, half, four.at[half, strip(0)], four.at[half, strip(0)], chips[j - 1]) for j in (1, 2, 3)
        ]
        copies["m", half] = [
            remote(21 + j, half, four.at[half, strip(4 - j)], last.at[half, strip(4 - j)], mate) for j in range(4)
        ]

    def go(name, half):
        for copy in copies[name, half]:
            copy.start()

    def arrived(name, half):
        for copy in copies[name, half]:
            copy.wait_recv()

    for half in range(2):
        go("c", half)
    for half in range(2):
        arrived("c", half)
        one[half] = (part[my_half, halves[half]].astype(F32) + rc[half].astype(F32)).astype(BF16)
        go("x", half)
    for half in range(2):
        arrived("x", half)
        total = one[half, strip(0), :].astype(F32)
        for j in range(3):
            total = total + rx[half, j].astype(F32)
        for j in range(8):
            two[half, j] = total[4 * j : 4 * j + 4]
        go("p", half)
    for half in range(2):
        arrived("p", half)
        total = two[half, sy]
        for j in range(7):
            total = total + ry[half, j]
        three[half, sy] = total
        go("g", half)
    for half in range(2):
        arrived("g", half)
        for j in range(8):
            strip32[pl.ds(4 * j, 4), :] = three[half, j]
        four[half, strip(0), :] = strip32[...].astype(BF16)
        go("w", half)
        copies["m", half][0].start()
    for half in range(2):
        for j in (1, 3, 2):
            copies["w", half][j - 1].wait_recv()
            copies["m", half][j].start()
        out[my_half, halves[half]] = four[half].astype(F32)
    for half in range(2):
        arrived("m", half)
        out[its_half, halves[half]] = last[half].astype(F32)
    for group in copies.values():
        for copy in group:
            copy.wait_send()


def combine(part):
    vm = pl.BlockSpec(memory_space=pltpu.VMEM)
    dma = pltpu.SemaphoreType.DMA
    return pl.pallas_call(
        combine_kernel,
        name="combine",
        out_shape=pltpu.VMEM((IMAGES, D), F32),
        in_specs=[vm],
        out_specs=vm,
        scratch_shapes=[
            pltpu.VMEM((2, 128, HALF), BF16),
            pltpu.VMEM((2, 128, HALF), BF16),
            pltpu.VMEM((2, 3, 32, HALF), BF16),
            pltpu.VMEM((2, 8, 4, HALF), F32),
            pltpu.VMEM((2, 7, 4, HALF), F32),
            pltpu.VMEM((2, 8, 4, HALF), F32),
            pltpu.VMEM((32, HALF), F32),
            pltpu.VMEM((2, 128, HALF), BF16),
            pltpu.VMEM((2, 128, HALF), BF16),
            dma((50,)),
            dma((50,)),
        ],
        compiler_params=pltpu.CompilerParams(
            collective_id=1, has_side_effects=True, vmem_limit_bytes=8 * MIB
        ),
    )(held(part))


def shards(tokens, lengths, ln_gain, w_qkv, w_out):
    rows = tokens.reshape(N, D)
    q, k, v, w_other = gather(rows, ln_gain, w_qkv, w_out)
    hidden, part = attend(lengths, q, k, v, w_other, rows, w_out)
    pooled = combine(part)
    return hidden.reshape(1, N, D), pooled.reshape(1, IMAGES, D)


def solution(mesh):
    in_specs = (P("dp", ("sx", "sy"), None), P("dp", None), P(), P("dp", None), P("dp", None))
    out_specs = (P("dp", ("sx", "sy"), None), P("dp", None, None))
    return jax.shard_map(shards, mesh=mesh, in_specs=in_specs, out_specs=out_specs, check_vma=False)
```

```python
import math

import jax
import jax.numpy as jnp
from jax import lax
from jax.experimental import pallas as pl
from jax.experimental.pallas import tpu as pltpu
from jax.sharding import PartitionSpec as P

MESH = pl.DeviceIdType.MESH
F32 = jnp.float32
BF16 = jnp.bfloat16
D = 1280
HALF = 640
N = 512
SIZE = 80
IMAGES = 256
TOTAL = 32768
SCALE = SIZE**-0.5 * math.log2(math.e)
PIECE = 80
CLASSES = (2, 3, 4, 5, 6, 9)
MIB = 1024 * 1024


def places():
    sx, sy, d = lax.axis_index("sx"), lax.axis_index("sy"), lax.axis_index("dp")
    h = lax.rem(sy, 2)
    flip = sy + 1 - 2 * h
    shard = sx * 8 + sy
    onward = lax.rem(shard + 2 - 4 * h + 64, 64)
    back = lax.rem(shard - 2 + 4 * h + 64, 64)
    mate = sx + 1 - 2 * lax.rem(sx, 2)
    where = {
        "a": (sx, sy, 1 - d),
        "b": (sx, flip, 1 - d),
        "xp": (lax.rem(sx + 2, 8), sy, d),
        "xm": (lax.rem(sx + 6, 8), sy, d),
        "core": (mate, sy, d),
        "z": (onward // 8, lax.rem(onward, 8), d),
        "zb": (back // 8, lax.rem(back, 8), d),
        "zi": (sx, lax.rem(sy + 6 + 4 * h, 8), d),
        "zj": (sx, lax.rem(sy + 10 - 4 * h, 8), d),
    }
    z = sy // 2
    first, last = (3 - z) // 3, z // 3
    where["hop"] = (6 - 4 * h * first, 2 + 4 * (1 - h) * last)
    return sx, sy, d, h, mate, where


def normalize(rows, gain):
    values = rows.astype(F32)
    center = values - jnp.mean(values, axis=-1, keepdims=True)
    spread = jnp.mean(center * center, axis=-1, keepdims=True)
    return (center * lax.rsqrt(spread + 1e-05) * gain).astype(BF16)


class Exchange:
    def __init__(self, own, other, sx, z, turn, where, send, recv):
        self.own, self.other, self.sx, self.z, self.turn = own, other, sx, z, turn
        self.where, self.send, self.recv = where, send, recv

    def copy(self, kind, t, side):
        pair = lax.rem(self.z + self.turn * (t - (kind == 8)) + 8, 4)
        chunk = pair + 3 + pair // 3 if side else pair + 3 * (pair // 3)
        cols = pl.ds(pl.multiple_of(chunk * HALF, 128), HALF)
        own, other, where = self.own, self.other, self.where
        hop = where["hop"][side] if t else (6, 2)[side]
        ahead, src, to = (
            (0, own, where["b" if side else "a"]),
            (0, other, where["xp"]),
            (0, other, where["xm"]),
            (0, other, where["core"]),
            (8 - hop, other, (lax.rem(self.sx + hop, 8),) + where["core"][1:]),
            (2, other, where["core"]),
            (6, other, where["core"]),
            (4, other, where["core"]),
            (0, other, where["zi"]),
        )[kind]
        rows = pl.ds(pl.multiple_of(lax.rem(self.sx + ahead, 8) * PIECE, 16), PIECE)
        i = kind * 8 + side * 4 + t
        return pltpu.make_async_remote_copy(
            src_ref=src.at[rows, cols],
            dst_ref=other.at[rows, cols],
            send_sem=self.send.at[i],
            recv_sem=self.recv.at[i],
            device_id=to,
            device_id_type=MESH,
        )

    def begin(self):
        for side in range(2):
            self.copy(0, 0, side).start()

    def landed(self, t):
        for side in range(2):
            self.copy(8 if t else 0, t, side).wait_recv()
            if t < 3:
                self.copy(8, t + 1, side).start()
            for kind in (1, 2, 3):
                self.copy(kind, t, side).start()

    def from_x(self, t):
        for side in range(2):
            for kind in (1, 2):
                self.copy(kind, t, side).wait_recv()
            for kind in (4, 5, 6):
                self.copy(kind, t, side).start()

    def from_far(self, t):
        for side in range(2):
            self.copy(4, t, side).wait_recv()
            self.copy(7, t, side).start()

    def finish(self):
        for t in range(4):
            for side in range(2):
                for kind in (3, 5, 6, 7):
                    self.copy(kind, t, side).wait_recv()

    def sent(self):
        for side in range(2):
            for t in range(4):
                for kind in range(1, 8):
                    self.copy(kind, t, side).wait_send()
                self.copy(8 if t else 0, t, side).wait_send()


class Halo:
    def __init__(self, tok, ta, tb, near, far, where, send, recv):
        self.table = []
        for i in range(4):
            self.table += [(tok, i, ta, i, "a"), (tok, 4 + i, tb, i, "b")]
        for i in range(4):
            self.table += [(ta, i, near, i, "b"), (tb, i, near, 4 + i, "a")]
        for i in range(4):
            self.table += [(near, i, far, i, "z"), (near, 4 + i, far, 4 + i, "z")]
        self.where, self.send, self.recv = where, send, recv

    def copy(self, i):
        src, at, dst, to, name = self.table[i]
        return pltpu.make_async_remote_copy(
            src_ref=src.at[pl.ds(64 * at, 64)],
            dst_ref=dst.at[pl.ds(64 * to, 64)],
            send_sem=self.send.at[i],
            recv_sem=self.recv.at[i],
            device_id=self.where[name],
            device_id_type=MESH,
        )

    def own(self, i):
        self.copy(2 * i).start()
        self.copy(2 * i + 1).start()

    def relay(self, i):
        for j in (2 * i, 2 * i + 1):
            self.copy(j).wait_recv()
            self.copy(8 + j).start()

    def onward(self, i):
        for j in (2 * i, 2 * i + 1):
            self.copy(8 + j).wait_recv()
            self.copy(16 + j).start()

    def arrived(self, i):
        for j in (2 * i, 2 * i + 1):
            self.copy(16 + j).wait_recv()

    def sent(self):
        for i in range(24):
            self.copy(i).wait_send()


def gather_kernel(
    tok_hbm, gain_ref, wq_hbm, wo_hbm,
    qs, ks, vs, wall,
    tok, wown, near, far, ta, tb, nrm, nrmh, acc, acch,
    w_send, w_recv, h_send, h_recv, local,
):
    sx, sy, d, h, mate, where = places()
    wq_in = pltpu.make_async_copy(wq_hbm, wown.at[:, pl.ds(0, 3 * D)], local.at[1])
    wo_in = pltpu.make_async_copy(wo_hbm, wown.at[:, pl.ds(3 * D, D)], local.at[2])
    tok_in = pltpu.make_async_copy(tok_hbm, tok, local.at[0])
    wq_in.start()
    wo_in.start()
    tok_in.start()
    barrier = pltpu.get_barrier_semaphore()
    partners = ("a", "b", "xp", "xm", "core", "z", "zb", "zi", "zj")
    for name in partners:
        pl.semaphore_signal(barrier, inc=1, device_id=where[name], device_id_type=MESH)
    wq_in.wait()
    wo_in.wait()
    pl.semaphore_wait(barrier, len(partners))

    weights = Exchange(wown, wall, sx, sy // 2, 1 - 2 * h, where, w_send, w_recv)
    halo = Halo(tok_hbm, ta, tb, near, far, where, h_send, h_recv)
    gain = gain_ref[...].reshape(1, D)
    mine = pl.ds(pl.multiple_of(d * HALF, 128), HALF)
    others = pl.ds(pl.multiple_of((1 - d) * HALF, 128), HALF)
    near_at = (1 - h) * (2 * N)
    far_at = h * (2 * N)

    def norm_own(i, _):
        rows = pl.ds(pl.multiple_of(i * 64, 64), 64)
        nrm[rows, :] = normalize(tok[rows, :], gain)
        return 0

    def first_half(part):
        def one(i, _):
            rows = pl.ds(pl.multiple_of(i * 256, 256), 256)
            cols = pl.ds(part * D, D)
            acc[rows, cols] = jnp.dot(nrm[rows, mine], wown[:, cols], preferred_element_type=F32)
            return 0

        lax.fori_loop(0, 2, one, 0)

    def second_half(i, _):
        rows = pl.ds(pl.multiple_of(i * 256, 256), 256)
        into = pl.ds(pl.multiple_of(N + i * 256, 256), 256)
        for part, ref, at, factor in ((0, qs, rows, SCALE), (1, ks, into, None), (2, vs, into, None)):
            cols = pl.ds(part * D, D)
            value = acc[rows, cols] + jnp.dot(nrm[rows, others], wall[:, cols], preferred_element_type=F32)
            if factor is not None:
                value = value * factor
            ref[at, :] = value.astype(BF16)
        return 0

    def halo_first(src, first, group):
        def one(j, _):
            at = pl.multiple_of(128 * first + 64 * lax.rem(j, 2) + 256 * (j // 2), 64)
            to = pl.multiple_of(256 * group + 64 * j, 64)
            nrmh[pl.ds(to, 64), :] = normalize(src[pl.ds(at, 64), :], gain)
            return 0

        lax.fori_loop(0, 4, one, 0)
        rows = pl.ds(256 * group, 256)
        for part in range(2):
            acch[rows, pl.ds(part * D, D)] = jnp.dot(
                nrmh[rows, mine], wown[:, pl.ds((part + 1) * D, D)], preferred_element_type=F32
            )

    def halo_second(first, base, group):
        rows = pl.ds(256 * group, 256)
        for part, ref in ((0, ks), (1, vs)):
            value = acch[rows, pl.ds(part * D, D)] + jnp.dot(
                nrmh[rows, others], wall[:, pl.ds((part + 1) * D, D)], preferred_element_type=F32
            )
            for j in range(2):
                start = pl.multiple_of(base + 128 * first + 256 * j, 128)
                ref[pl.ds(start, 128), :] = value[128 * j : 128 * j + 128].astype(BF16)

    def halo_whole(src, first, base):
        for j in range(4):
            at = 128 * first + 64 * (j % 2) + 256 * (j // 2)
            nrmh[pl.ds(64 * j, 64), :] = normalize(src[pl.ds(at, 64), :], gain)
        rows = pl.ds(0, 256)
        for part, ref in ((1, ks), (2, vs)):
            cols = pl.ds(part * D, D)
            value = jnp.dot(nrmh[rows, mine], wown[:, cols], preferred_element_type=F32)
            value = value + jnp.dot(nrmh[rows, others], wall[:, cols], preferred_element_type=F32)
            for j in range(2):
                start = pl.multiple_of(base + 128 * first + 256 * j, 128)
                ref[pl.ds(start, 128), :] = value[128 * j : 128 * j + 128].astype(BF16)

    with jax.named_scope("g0"):
        weights.begin()
        halo.own(0)
        halo.own(1)
        tok_in.wait()
        lax.fori_loop(0, N // 64, norm_own, 0)
        weights.landed(0)
        first_half(0)
    with jax.named_scope("g1"):
        halo.relay(0)
        halo.own(2)
        first_half(1)
        weights.landed(1)
    with jax.named_scope("g2"):
        halo.relay(1)
        halo.own(3)
        first_half(2)
        weights.landed(2)
    with jax.named_scope("g3"):
        halo.onward(0)
        weights.from_x(0)
        weights.landed(3)
    with jax.named_scope("g4"):
        halo.relay(2)
        weights.from_x(1)
        halo.onward(1)
        weights.from_x(2)
    with jax.named_scope("g5"):
        halo_first(near, 0, 0)
        halo.relay(3)
    with jax.named_scope("g6"):
        weights.from_far(0)
        weights.from_x(3)
        halo.onward(2)
        weights.from_far(1)
        halo.onward(3)
    with jax.named_scope("g7"):
        weights.from_far(2)
        halo_first(near, 1, 1)
    with jax.named_scope("g8"):
        weights.from_far(3)
        halo.arrived(0)
        halo.arrived(1)
        halo_first(far, 0, 2)
        weights.finish()
    with jax.named_scope("g9"):
        lax.fori_loop(0, 2, second_half, 0)
        halo_second(0, near_at, 0)
        halo_second(1, near_at, 1)
        halo_second(0, far_at, 2)
    with jax.named_scope("g12"):
        halo.arrived(2)
        halo.arrived(3)
    with jax.named_scope("g13"):
        halo_whole(far, 1, far_at)
        weights.sent()
        halo.sent()


def held(x):
    return pltpu.with_memory_space_constraint(x, pltpu.VMEM)


def outside(x):
    return pltpu.with_memory_space_constraint(x, pltpu.HBM)


def gather(tokens, gain, w_qkv, w_out):
    any_ = pl.BlockSpec(memory_space=pltpu.HBM)
    vm = pl.BlockSpec(memory_space=pltpu.VMEM)
    dma = pltpu.SemaphoreType.DMA
    return pl.pallas_call(
        gather_kernel,
        name="gather",
        out_shape=(
            pltpu.VMEM((N, D), BF16),
            pltpu.VMEM((3 * N, D), BF16),
            pltpu.VMEM((3 * N, D), BF16),
            pltpu.VMEM((HALF, 4 * D), BF16),
        ),
        in_specs=[any_, vm, any_, any_],
        out_specs=(vm,) * 4,
        scratch_shapes=[
            pltpu.VMEM((N, D), BF16),
            pltpu.VMEM((HALF, 4 * D), BF16),
            pltpu.VMEM((N, D), BF16),
            pltpu.VMEM((N, D), BF16),
            pltpu.VMEM((256, D), BF16),
            pltpu.VMEM((256, D), BF16),
            pltpu.VMEM((N, D), BF16),
            pltpu.VMEM((768, D), BF16),
            pltpu.VMEM((N, 3 * D), F32),
            pltpu.VMEM((768, 2 * D), F32),
            dma((72,)),
            dma((72,)),
            dma((24,)),
            dma((24,)),
            dma((3,)),
        ],
        compiler_params=pltpu.CompilerParams(
            collective_id=0, has_side_effects=True, vmem_limit_bytes=44 * MIB
        ),
    )(outside(tokens), gain, outside(w_qkv), outside(w_out))


def attend_kernel(
    lens_ref, q, k, v, wb, tok_hbm, wa_hbm,
    hid_hbm, part_ref,
    tok, wa, ctx, bias, hid, qid, kid, sems,
):
    sx, sy, d = lax.axis_index("sx"), lax.axis_index("sy"), lax.axis_index("dp")
    copies = [
        pltpu.make_async_copy(a, b, sems.at[i])
        for i, (a, b) in enumerate(
            ((tok_hbm, tok), (wa_hbm, wa))
        )
    ]
    for copy in copies:
        copy.start()
    first = (sx * 8 + sy) * N
    base = first - N

    lens = lens_ref[...].astype(F32)
    down = lax.broadcasted_iota(jnp.int32, (IMAGES, IMAGES), 0)
    along = lax.broadcasted_iota(jnp.int32, (IMAGES, IMAGES), 1)
    wide = jnp.broadcast_to(lens, (IMAGES, IMAGES))
    off_col = jnp.sum(jnp.where(along < down, wide, 0.0), axis=1, keepdims=True)
    len_col = jnp.sum(jnp.where(along == down, wide, 0.0), axis=1, keepdims=True)
    off_row = jnp.sum(
        jnp.where(down < along, jnp.broadcast_to(len_col, (IMAGES, IMAGES)), 0.0), axis=0, keepdims=True
    )
    for j in range(3):
        pos = (lax.broadcasted_iota(jnp.int32, (1, N), 1) + (base + j * N)).astype(F32)
        count = jnp.sum(jnp.where(off_col <= pos, 1.0, 0.0), axis=0, keepdims=True) - 1.0
        kid[:, pl.ds(j * N, N)] = jnp.where(pos < TOTAL, count, -1.0)
    for j in range(4):
        pos = (lax.broadcasted_iota(jnp.int32, (128, 1), 0) + (first + j * 128)).astype(F32)
        qid[pl.ds(j * 128, 128), :] = jnp.sum(jnp.where(off_row <= pos, 1.0, 0.0), axis=1, keepdims=True) - 1.0

    def block(i, _):
        rows = pl.ds(pl.multiple_of(i * 128, 128), 128)
        begin = (first + i * 128).astype(F32)
        low = jnp.max(jnp.where(off_row <= begin, off_row, 0.0)).astype(jnp.int32)
        high = jnp.min(jnp.where(off_row > begin + 127.0, off_row, float(TOTAL))).astype(jnp.int32)
        low = (low - base) >> 7
        high = (high - base + 127) >> 7
        blocks = high - low
        ids = qid[rows, :]
        before = 0
        for size in CLASSES:
            n = size * 128

            @pl.when((blocks > before) & (blocks <= size))
            def _():
                start = pl.multiple_of(jnp.minimum(low, 12 - size) * 128, 128)
                keys = pl.ds(start, n)
                bias[:, pl.ds(0, n)] = jnp.where(ids == kid[:, keys], 0.0, -1e30)

                several = 8

                def pairs(group, _):
                    work, soft = {}, {}

                    def first(sub):
                        pair = group * several + sub
                        tile = (pair * 5) >> 2
                        lanes = pl.ds(pl.multiple_of(tile * 128, 128), 256)
                        shift = pair * 160 - tile * 128
                        lane = lax.broadcasted_iota(jnp.int32, (1, 256), 1) - shift
                        one = (lane >= 0) & (lane < SIZE)
                        two = (lane >= SIZE) & (lane < 2 * SIZE)
                        window = q[rows, lanes]
                        both = jnp.concatenate(
                            [
                                window * jnp.where(one, 1.0, 0.0).astype(BF16),
                                window * jnp.where(two, 1.0, 0.0).astype(BF16),
                            ],
                            axis=0,
                        )
                        scores = lax.dot_general(
                            both, k[keys, lanes], (((1,), (1,)), ((), ())), preferred_element_type=F32
                        )
                        extra = bias[:, pl.ds(0, n)]
                        scores = scores + jnp.concatenate([extra, extra], axis=0)
                        work[sub] = (lanes, one, two, scores, jnp.max(scores, axis=1, keepdims=True))

                    def middle(sub):
                        lanes, one, two, scores, top = work.pop(sub)
                        weights = jnp.exp2(scores - top)
                        total = jnp.sum(weights, axis=1, keepdims=True)
                        soft[sub] = (lanes, one, two, weights.astype(BF16), total)

                    def final(sub):
                        lanes, one, two, weights, total = soft.pop(sub)
                        mixed = jnp.dot(weights, v[keys, lanes], preferred_element_type=F32) * (1.0 / total)
                        old = ctx[rows, lanes].astype(F32)
                        ctx[rows, lanes] = jnp.where(one, mixed[:128], jnp.where(two, mixed[128:], old)).astype(BF16)

                    first(0)
                    for sub in range(several):
                        if sub + 1 < several:
                            first(sub + 1)
                        middle(sub)
                        if sub:
                            final(sub - 1)
                    final(several - 1)
                    return 0

                lax.fori_loop(0, 8 // several, pairs, 0)

            before = size
        return 0

    lax.fori_loop(0, 4, block, 0)
    for copy in copies:
        copy.wait()
    mine = pl.ds(pl.multiple_of(d * HALF, 128), HALF)
    others = pl.ds(pl.multiple_of((1 - d) * HALF, 128), HALF)

    def project(i, _):
        rows = pl.ds(pl.multiple_of(i * 256, 256), 256)
        mixed = jnp.dot(ctx[rows, mine], wa[...], preferred_element_type=F32)
        mixed = mixed + jnp.dot(ctx[rows, others], wb[:, pl.ds(3 * D, D)], preferred_element_type=F32)
        hid[rows, :] = (tok[rows, :].astype(F32) + mixed).astype(BF16)
        return 0

    lax.fori_loop(0, 2, project, 0)
    out = pltpu.make_async_copy(hid, hid_hbm, sems.at[2])
    out.start()
    image = lax.broadcasted_iota(jnp.int32, (IMAGES, 1), 0).astype(F32)
    onehot = jnp.where(image == kid[:, pl.ds(N, N)], 1.0, 0.0).astype(BF16)
    sums = jnp.dot(onehot, hid[...], preferred_element_type=F32)
    part_ref[...] = (sums / len_col).astype(BF16)
    out.wait()


def attend(lengths, q, k, v, w_other, tokens, w_own):
    any_ = pl.BlockSpec(memory_space=pltpu.HBM)
    vm = pl.BlockSpec(memory_space=pltpu.VMEM)
    return pl.pallas_call(
        attend_kernel,
        name="attend",
        out_shape=(
            jax.ShapeDtypeStruct((N, D), BF16),
            pltpu.VMEM((IMAGES, D), BF16),
        ),
        in_specs=[vm] * 5 + [any_] * 2,
        out_specs=(any_, vm),
        scratch_shapes=[
            pltpu.VMEM((N, D), BF16),
            pltpu.VMEM((HALF, D), BF16),
            pltpu.VMEM((N, D), BF16),
            pltpu.VMEM((128, 128 * CLASSES[-1]), F32),
            pltpu.VMEM((N, D), BF16),
            pltpu.VMEM((N, 1), F32),
            pltpu.VMEM((1, 3 * N), F32),
            pltpu.SemaphoreType.DMA((3,)),
        ],
        compiler_params=pltpu.CompilerParams(vmem_limit_bytes=28 * MIB),
    )(lengths, *[held(x) for x in (q, k, v, w_other)], outside(tokens), outside(w_own))


def combine_kernel(part, out, rc, one, rx, two, ry, three, strip32, four, last, send, recv):
    sx, sy, d = lax.axis_index("sx"), lax.axis_index("sy"), lax.axis_index("dp")
    core = lax.rem(sx, 2)
    chip = sx // 2
    mate = (sx + 1 - 2 * core, sy, d)
    chips = [(lax.rem(sx + 2 * j, 8), sy, d) for j in (1, 2, 3)]
    plane = [(sx, lax.rem(sy + j, 8), d) for j in range(1, 8)]
    barrier = pltpu.get_barrier_semaphore()
    for who in [mate] + chips + plane:
        pl.semaphore_signal(barrier, inc=1, device_id=who, device_id_type=MESH)
    pl.semaphore_wait(barrier, 11)

    my_half = pl.ds(pl.multiple_of(core * 128, 128), 128)
    its_half = pl.ds(pl.multiple_of((1 - core) * 128, 128), 128)
    halves = [pl.ds(half * HALF, HALF) for half in range(2)]

    def strip(ahead):
        return pl.ds(pl.multiple_of(lax.rem(chip + ahead, 4) * 32, 32), 32)

    def remote(i, half, src, dst, who):
        return pltpu.make_async_remote_copy(
            src_ref=src,
            dst_ref=dst,
            send_sem=send.at[25 * half + i],
            recv_sem=recv.at[25 * half + i],
            device_id=who,
            device_id_type=MESH,
        )

    copies = {}
    for half in range(2):
        copies["c", half] = [remote(0, half, part.at[its_half, halves[half]], rc.at[half], mate)]
        copies["x", half] = [
            remote(j, half, one.at[half, strip(j)], rx.at[half, j - 1], chips[j - 1]) for j in (1, 2, 3)
        ]
        copies["p", half] = [
            remote(3 + j, half, two.at[half, lax.rem(sy + j, 8)], ry.at[half, j - 1], plane[j - 1])
            for j in range(1, 8)
        ]
        copies["g", half] = [
            remote(10 + j, half, three.at[half, sy], three.at[half, sy], plane[j - 1]) for j in range(1, 8)
        ]
        copies["w", half] = [
            remote(17 + j, half, four.at[half, strip(0)], four.at[half, strip(0)], chips[j - 1]) for j in (1, 2, 3)
        ]
        copies["m", half] = [
            remote(21 + j, half, four.at[half, strip(4 - j)], last.at[half, strip(4 - j)], mate) for j in range(4)
        ]

    def go(name, half):
        for copy in copies[name, half]:
            copy.start()

    def arrived(name, half):
        for copy in copies[name, half]:
            copy.wait_recv()

    for half in range(2):
        go("c", half)
    for half in range(2):
        arrived("c", half)
        one[half] = (part[my_half, halves[half]].astype(F32) + rc[half].astype(F32)).astype(BF16)
        go("x", half)
    for half in range(2):
        arrived("x", half)
        total = one[half, strip(0), :].astype(F32)
        for j in range(3):
            total = total + rx[half, j].astype(F32)
        for j in range(8):
            two[half, j] = total[4 * j : 4 * j + 4]
        go("p", half)
    for half in range(2):
        arrived("p", half)
        total = two[half, sy]
        for j in range(7):
            total = total + ry[half, j]
        three[half, sy] = total
        go("g", half)
    for half in range(2):
        arrived("g", half)
        for j in range(8):
            strip32[pl.ds(4 * j, 4), :] = three[half, j]
        four[half, strip(0), :] = strip32[...].astype(BF16)
        go("w", half)
        copies["m", half][0].start()
    for half in range(2):
        for j in (1, 3, 2):
            copies["w", half][j - 1].wait_recv()
            copies["m", half][j].start()
        out[my_half, halves[half]] = four[half].astype(F32)
    for half in range(2):
        arrived("m", half)
        out[its_half, halves[half]] = last[half].astype(F32)
    for group in copies.values():
        for copy in group:
            copy.wait_send()


def combine(part):
    vm = pl.BlockSpec(memory_space=pltpu.VMEM)
    dma = pltpu.SemaphoreType.DMA
    return pl.pallas_call(
        combine_kernel,
        name="combine",
        out_shape=pltpu.VMEM((IMAGES, D), F32),
        in_specs=[vm],
        out_specs=vm,
        scratch_shapes=[
            pltpu.VMEM((2, 128, HALF), BF16),
            pltpu.VMEM((2, 128, HALF), BF16),
            pltpu.VMEM((2, 3, 32, HALF), BF16),
            pltpu.VMEM((2, 8, 4, HALF), F32),
            pltpu.VMEM((2, 7, 4, HALF), F32),
            pltpu.VMEM((2, 8, 4, HALF), F32),
            pltpu.VMEM((32, HALF), F32),
            pltpu.VMEM((2, 128, HALF), BF16),
            pltpu.VMEM((2, 128, HALF), BF16),
            dma((50,)),
            dma((50,)),
        ],
        compiler_params=pltpu.CompilerParams(
            collective_id=1, has_side_effects=True, vmem_limit_bytes=8 * MIB
        ),
    )(held(part))


def shards(tokens, lengths, ln_gain, w_qkv, w_out):
    rows = tokens.reshape(N, D)
    q, k, v, w_other = gather(rows, ln_gain, w_qkv, w_out)
    hidden, part = attend(lengths, q, k, v, w_other, rows, w_out)
    pooled = combine(part)
    return hidden.reshape(1, N, D), pooled.reshape(1, IMAGES, D)


def solution(mesh):
    in_specs = (P("dp", ("sx", "sy"), None), P("dp", None), P(), P("dp", None), P("dp", None))
    out_specs = (P("dp", ("sx", "sy"), None), P("dp", None, None))
    return jax.shard_map(shards, mesh=mesh, in_specs=in_specs, out_specs=out_specs, check_vma=False)
```
